32 devices in a mesh: parts: 2 (over x), shot: 2 (over core), space: 8 (over z, y).
Axes of the slice: x: 2, y: 2, z: 4, core: 2. Of those that a mesh axis runs over, the one named last changes fastest.
Arguments:
- image: float32 [3200, 2, 192], P(('parts', 'space')), parts along dimension 0, may hold values from -6 to 6
- coil_maps: bfloat16 [16, 3200, 2, 192], P(None, ('parts', 'space')), parts along dimension 1, may hold values from -1.5 to 1.5
- psf_phase: float32 [3200, 576], P(('parts', 'space')), parts along dimension 0, may hold values from -3.140625 to 3.140625
- line_mask: int32 [4, 200], P(('parts', 'shot')), parts along dimension 0, may hold values 0 or 1
- motion: int32 [4, 3], P(('parts', 'shot')), parts along dimension 0, may hold values from 0 to 16
Outputs:
- result: float32 [3200, 2, 192], P(('parts', 'space')), parts along dimension 0
The draws below stay inside these ranges and needn't reach their ends.
There are 2 independent parts, one for each index of `parts`. The reference program is written for one: setup_inputs(seed, part) draws one part's arguments, and reference() takes and returns one part's arrays. A program takes and returns all parts, laid end to end along the dimension named above; each array names one. Nothing has to cross between parts.
Inputs may be any that keep to these rules, and one draw needn't show every extreme that they name: `motion`: column 0 selects the rotation angle, columns 1 and 2 the shifts along x and y.
All inputs are finite; a program needn't handle non-finite values. No bound on the sum of `line_mask` on one device may be relied on, other than what follows from the above.
Results may differ from the reference program's by a relative error of at most 0.003.
Values may be sent and summed in bfloat16 or wider, within the bound.
No kernel may reach another device: no remote copies, remote signals or barrier semaphores. Data moves between devices by JAX's collectives and lax.ppermute only.
A program may use at most 64 MiB of HBM per device.

```python
import jax
import jax.numpy as jnp
from jax import lax

NX = 192
NY = 200
COILS = 16
Z = 8
LEVELS = 17
NR = 576
SHOTS = 2


def place_ends(entries, key, smallest, high):
    spot = [jax.random.randint(jax.random.fold_in(key, axis), (), 0, length) for axis, length in enumerate(entries.shape)]
    widest = entries.shape.index(max(entries.shape))
    beside = spot[:widest] + [(spot[widest] + 1) % entries.shape[widest]] + spot[widest + 1:]
    return entries.at[tuple(spot)].set(smallest).at[tuple(beside)].set(high)


def level_of(own_key, shape, split, smallest, top_value):
    def one(axis_at, blocks):
        heights = jax.random.uniform(jax.random.fold_in(jax.random.fold_in(own_key, 6), axis_at), (blocks,), jnp.float32, smallest / len(split), top_value / len(split))
        return jnp.repeat(jnp.exp(heights), shape[axis_at] // blocks).reshape((-1,) + (1,) * (len(shape) - axis_at - 1))

    factor_of = one(*split[0])
    for cut in split[1:]:
        factor_of = factor_of * one(*cut)
    return factor_of


def scatter_about(key, extent, deviation, most, cuts=(), held_as=jnp.bfloat16):
    entries = deviation * jax.random.normal(key, extent, jnp.float32)
    if cuts:
        entries = entries * level_of(key, extent, cuts, -0.22, 0.18)
    return jnp.clip(entries, -most, most).astype(held_as)


def setup_inputs(seed: int = 0, part: int = 0) -> dict:
    splits = jax.random.split(jax.random.key(seed), 6)
    own_keys = jax.random.split(jax.random.fold_in(splits[5], part), 6)
    image = scatter_about(own_keys[0], (Z * NY, 2, NX), 1.0, 6.0, ((0, 8),), jnp.float32)
    coil_maps = scatter_about(own_keys[1], (COILS, Z * NY, 2, NX), COILS ** -0.5, 1.5, ((1, 8),))
    psf_phase = jnp.clip(jax.random.uniform(own_keys[2], (Z * NY, NR), jnp.float32, -3.140625, 3.140625), -3.140625, 3.140625)
    line_mask = place_ends((jax.random.randint(own_keys[3], (SHOTS, NY), 0, 3) < 1).astype(jnp.int32), jax.random.fold_in(own_keys[3], 1), 0, 1)
    motion = place_ends(jax.random.randint(own_keys[4], (SHOTS, 3), 0, LEVELS), jax.random.fold_in(own_keys[4], 1), 0, LEVELS - 1).astype(jnp.int32)
    return dict(image=image, coil_maps=coil_maps, psf_phase=psf_phase, line_mask=line_mask, motion=motion)


PRECISE = lax.Precision.HIGHEST
ANGLE_STEP = 0.02
SHIFT_STEP = 0.5


def dft_parts(size_in, size_out, modulus, sign):
    inputs = jnp.arange(size_in, dtype=jnp.int32)[:, None]
    outputs = jnp.arange(size_out, dtype=jnp.int32)[None, :]
    angle = ((inputs * outputs) % modulus).astype(jnp.float32) * (2.0 * jnp.pi / modulus)
    factor = float(modulus) ** -0.5
    return jnp.cos(angle) * factor, jnp.sin(angle) * (sign * factor)


def block(parts):
    real_part, imag_part = parts
    upper = jnp.concatenate([real_part, imag_part], 1)
    bottom = jnp.concatenate([-imag_part, real_part], 1)
    return jnp.concatenate([upper, bottom], 0)


def quad(real_part, imag_part):
    return jnp.stack([jnp.stack([real_part, -imag_part], 1), jnp.stack([imag_part, real_part], 1)], 0)


def signed_freq(length):
    counter = jnp.arange(length, dtype=jnp.int32)
    return jnp.where(counter < length // 2, counter, counter - length).astype(jnp.float32)


def turn_phase(values, phase):
    cosine = jnp.cos(phase)
    sine_part = jnp.sin(phase)
    real_part = values[..., 0, :]
    imag_part = values[..., 1, :]
    return jnp.stack([real_part * cosine - imag_part * sine_part, real_part * sine_part + imag_part * cosine], -2)


def complex_mul(left, right):
    return jnp.stack([left[..., 0, :] * right[..., 0, :] - left[..., 1, :] * right[..., 1, :],
                      left[..., 0, :] * right[..., 1, :] + left[..., 1, :] * right[..., 0, :]], -2)


def conj_mul(left, right):
    return jnp.stack([left[..., 0, :] * right[..., 0, :] + left[..., 1, :] * right[..., 1, :],
                      left[..., 0, :] * right[..., 1, :] - left[..., 1, :] * right[..., 0, :]], -2)


def shear_rows(values, shift, sign):
    length = values.shape[-1]
    lines = values.shape[0]
    forward = block(dft_parts(length, length, length, -1.0))
    inverse = block(dft_parts(length, length, length, 1.0))
    spectra = jnp.dot(values.reshape(lines, 2 * length), forward, precision=PRECISE, preferred_element_type=jnp.float32)
    phase = (sign * -2.0 * jnp.pi / length) * shift[:, None] * signed_freq(length)[None, :]
    spectra = turn_phase(spectra.reshape(lines, 2, length), phase)
    result = jnp.dot(spectra.reshape(lines, 2 * length), inverse, precision=PRECISE, preferred_element_type=jnp.float32)
    return result.reshape(lines, 2, length)


def shear_columns(values, shift, sign):
    length = values.shape[1]
    forward = quad(*dft_parts(length, length, length, -1.0))
    inverse = quad(*dft_parts(length, length, length, 1.0))
    spectra = jnp.einsum("oaib,zbix->zaox", forward, values, precision=PRECISE)
    phase = (sign * -2.0 * jnp.pi / length) * signed_freq(length)[:, None] * shift[None, :]
    spectra = turn_phase(spectra, phase)
    return jnp.einsum("oaib,zbix->zaox", inverse, spectra, precision=PRECISE)


def geometry(motion_row):
    offsets = motion_row.astype(jnp.float32) - (LEVELS - 1) / 2.0
    angle = offsets[0] * ANGLE_STEP
    return -jnp.tan(angle / 2.0), jnp.sin(angle), offsets[1] * SHIFT_STEP, offsets[2] * SHIFT_STEP


def rotate(values, motion_row, sign):
    slope, tilt, shift_x, shift_y = geometry(motion_row)
    lines = values.shape[0]
    width = values.shape[2]
    across = (jnp.arange(lines, dtype=jnp.int32) % NY).astype(jnp.float32) - NY / 2.0
    along = jnp.arange(width, dtype=jnp.int32).astype(jnp.float32) - width / 2.0

    def column_pass(current):
        view_slices = current.reshape(lines // NY, NY, 2, width)
        return shear_columns(view_slices, tilt * along + shift_y, sign).reshape(lines, 2, width)

    if sign > 0:
        current = shear_rows(values, slope * across + shift_x, 1.0)
        current = column_pass(current)
        return shear_rows(current, slope * across, 1.0)
    current = shear_rows(values, slope * across, -1.0)
    current = column_pass(current)
    return shear_rows(current, slope * across + shift_x, -1.0)


def line_table(mask_row):
    cosine, sine_part = dft_parts(NY, NY, NY, 1.0)
    weight = mask_row.astype(jnp.float32)[:, None]
    real_part = jnp.dot(cosine.T, weight * cosine, precision=PRECISE) + jnp.dot(sine_part.T, weight * sine_part, precision=PRECISE)
    imag_part = jnp.dot(sine_part.T, weight * cosine, precision=PRECISE) - jnp.dot(cosine.T, weight * sine_part, precision=PRECISE)
    return quad(real_part, imag_part).astype(jnp.bfloat16)


def reference(image, coil_maps, psf_phase, line_mask, motion):
    lines = image.shape[0]
    width = image.shape[2]
    readout = psf_phase.shape[1]
    pad_table = block(dft_parts(width, readout, readout, -1.0)).astype(jnp.bfloat16)
    crop_table = block(dft_parts(readout, width, readout, 1.0)).astype(jnp.bfloat16)

    def one_shot(running, inputs):
        mask_row, motion_row = inputs
        projector = line_table(mask_row).astype(jnp.float32)
        rotated = rotate(image, motion_row, 1)

        def one_coil(combined, coil):
            coil_values = coil.astype(jnp.float32)
            coil_image = complex_mul(coil_values, rotated).astype(jnp.bfloat16)
            spectra = jnp.dot(coil_image.reshape(lines, 2 * width), pad_table, preferred_element_type=jnp.float32)
            waved = turn_phase(spectra.reshape(lines, 2, readout), psf_phase).astype(jnp.bfloat16)
            view_slices = waved.reshape(lines // NY, NY, 2, readout).astype(jnp.float32)
            projected = jnp.einsum("oaib,zbik->zaok", projector, view_slices, precision=PRECISE).astype(jnp.bfloat16)
            unwaved = turn_phase(projected.reshape(lines, 2, readout).astype(jnp.float32), -psf_phase).astype(jnp.bfloat16)
            back = jnp.dot(unwaved.reshape(lines, 2 * readout), crop_table, preferred_element_type=jnp.float32)
            return combined + conj_mul(coil_values, back.reshape(lines, 2, width)), None

        combined, _ = lax.scan(one_coil, jnp.zeros(image.shape, jnp.float32), coil_maps)
        return running + rotate(combined, motion_row, -1), None

    result, _ = lax.scan(one_shot, jnp.zeros(image.shape, jnp.float32), (line_mask, motion))
    return result
```

```python
import functools

import jax
import jax.numpy as jnp
import numpy as np
from jax import lax
from jax.experimental import pallas as pl
from jax.experimental.pallas import tpu as pltpu
from jax.sharding import PartitionSpec as P

LEVELS = 17
ANGLE_STEP = 0.02
SHIFT_STEP = 0.5
LANES = 128
BF = jnp.bfloat16
F32 = jnp.float32


def split_pair(table):
    high = table.astype(np.float32).astype(BF)
    low = (table - high.astype(np.float64)).astype(np.float32).astype(BF)
    return np.stack([high, low])


def row_tables(width):
    index = np.arange(width)
    angle = 2 * np.pi * (np.outer(index, index) % width) / width
    return split_pair(np.concatenate([np.cos(angle), np.sin(angle)], 0) / np.sqrt(width))


def column_tables(length):
    half = length // 2
    result = []
    for parity in range(2):
        inputs = np.arange(half)[:, None]
        freqs = 2 * np.arange(half)[None, :] + parity
        angle = -2 * np.pi * (inputs * freqs % length) / length
        wave = np.exp(1j * angle) / np.sqrt(length)
        table = np.zeros((2 * LANES, 2 * LANES))
        table[:half, :half] = wave.real
        table[:half, LANES:LANES + half] = wave.imag
        table[LANES:LANES + half, :half] = -wave.imag
        table[LANES:LANES + half, LANES:LANES + half] = wave.real
        result.append(split_pair(table))
    return np.stack(result)


def readout_tables(width, readout):
    half = width // 2
    classes = readout // half
    pads, crops = [], []
    for j in range(classes):
        k = np.arange(half)[:, None] * classes + j
        x = np.arange(half)[None, :]
        angle = -2 * np.pi * (k * x % readout) / readout
        cosine = (np.cos(angle) / np.sqrt(readout)).astype(np.float32).astype(BF)
        sine = (np.sin(angle) / np.sqrt(readout)).astype(np.float32).astype(BF)
        table = np.block([[cosine, -sine], [sine, cosine]])
        pads.append(table)
        crops.append(table.T)
    return np.stack(pads), np.stack(crops)


def turn_polys():
    nodes = np.cos(np.pi * (np.arange(400) + 0.5) / 400) * 0.125 + 0.125
    root = np.sqrt(nodes)
    out = []
    for value in (np.cos(2 * np.pi * root), np.sin(2 * np.pi * root) / root):
        series = np.polynomial.chebyshev.Chebyshev.fit(nodes, value, 6, domain=[0, 0.25])
        out.append([float(c) for c in series.convert(kind=np.polynomial.Polynomial).coef])
    return out


COS_POLY, SIN_POLY = turn_polys()


def turn_pair(turns):
    square = turns * turns
    cosine = jnp.full_like(square, COS_POLY[-1])
    sine = jnp.full_like(square, SIN_POLY[-1])
    for c, s in zip(COS_POLY[-2::-1], SIN_POLY[-2::-1]):
        cosine = cosine * square + c
        sine = sine * square + s
    return cosine, sine * turns


def wrap(turns):
    return turns - jnp.floor(turns + 0.5)


def dot(left, right):
    return jnp.dot(left, right, preferred_element_type=F32)


def dot_nt(left, right):
    return lax.dot_general(left, right, (((1,), (1,)), ((), ())), preferred_element_type=F32)


def two(value):
    high = value.astype(BF)
    return high, (value - high.astype(F32)).astype(BF)


def spread(value, length):
    half = length // 2
    blank = jnp.zeros((value.shape[0], LANES - half), value.dtype)
    return jnp.concatenate([value[:, :half], blank, value[:, half:], blank], 1)


def table_rows(tx_ref, value):
    high, low = two(value)
    return dot(tx_ref[0], high) + dot(tx_ref[1], high) + dot(tx_ref[0], low)


def shear_rows(re, im, tx_ref, phase_ref, sign):
    width = re.shape[0]
    from_re, from_im = table_rows(tx_ref, re), table_rows(tx_ref, im)
    sr = from_re[:width] + from_im[width:]
    si = from_im[:width] - from_re[width:]
    c, s = phase_ref[0], phase_ref[1] * sign
    from_re, from_im = table_rows(tx_ref, sr * c - si * s), table_rows(tx_ref, sr * s + si * c)
    return from_re[:width] - from_im[width:], from_im[:width] + from_re[width:]


def shear_columns(re, im, ty_ref, phase_ref, sign):
    back = []
    for parity in range(2):
        join = (lambda v: v[:, :LANES] - v[:, LANES:]) if parity else (lambda v: v[:, :LANES] + v[:, LANES:])
        high, low = two(jnp.concatenate([join(re), join(im)], 1))
        th, tl = ty_ref[parity, 0], ty_ref[parity, 1]
        spectra = dot(high, th) + dot(low, th) + dot(high, tl)
        sr, si = spectra[:, :LANES], spectra[:, LANES:]
        c, s = phase_ref[2 * parity], phase_ref[2 * parity + 1] * sign
        high, low = two(jnp.concatenate([sr * c - si * s, sr * s + si * c], 1))
        back.append(dot_nt(high, th) + dot_nt(low, th) + dot_nt(high, tl))
    even, odd = back
    low_half, high_half = even + odd, even - odd
    return (
        jnp.concatenate([low_half[:, :LANES], high_half[:, :LANES]], 1),
        jnp.concatenate([low_half[:, LANES:], high_half[:, LANES:]], 1),
    )


def signed(counter, length):
    return jnp.where(counter < length // 2, counter, counter - length).astype(F32)


def make_phases(motion_ref, p1_ref, pc_ref, p3_ref, width, length):
    half = length // 2
    center = (LEVELS - 1) / 2.0
    shift_x = (motion_ref[0, 1].astype(F32) - center) * SHIFT_STEP
    shift_y = (motion_ref[0, 2].astype(F32) - center) * SHIFT_STEP
    angle = jnp.full((8, LANES), (motion_ref[0, 0].astype(F32) - center) * ANGLE_STEP, F32)
    tilt = jnp.sin(angle)[:1, :1]
    slope = -(jnp.sin(angle * 0.5) / jnp.cos(angle * 0.5))[:1, :1]
    lane = lax.broadcasted_iota(jnp.int32, (1, 2 * LANES), 1)
    line = jnp.where(lane < LANES, lane, lane - LANES + half)
    bend = slope * (line.astype(F32) - length / 2.0)
    freq = signed(lax.broadcasted_iota(jnp.int32, (width, 1), 0), width) * (-1.0 / width)
    for ref, shift in ((p1_ref, bend + shift_x), (p3_ref, bend)):
        c, s = turn_pair(wrap(freq * shift))
        ref[0] = c
        ref[1] = s
    along = lax.broadcasted_iota(jnp.int32, (width, 1), 0).astype(F32) - width / 2.0
    shift = tilt * along + shift_y
    lane = lax.broadcasted_iota(jnp.int32, (1, LANES), 1)
    for parity in range(2):
        freq = signed(2 * lane + parity, length) * (-1.0 / length)
        c, s = turn_pair(wrap(shift * freq))
        pc_ref[2 * parity] = c
        pc_ref[2 * parity + 1] = s


def make_projector(mask_ref, ty_ref, h_ref, length):
    half = length // 2
    mask = jnp.broadcast_to(mask_ref[...].astype(F32), (8, length)).astype(BF)
    line = lax.broadcasted_iota(jnp.int32, (length, 2 * LANES), 0)
    lane = lax.broadcasted_iota(jnp.int32, (length, 2 * LANES), 1) % LANES
    picked = []
    for parity in range(2):
        select = jnp.where((line == 2 * lane + parity) & (lane < half), 1.0, 0.0).astype(BF)
        picked.append(dot(mask, select)[:1])
    counts = [jnp.sum(p[:, :LANES], 1, keepdims=True) for p in picked]
    total = ((counts[0] + counts[1]) / length).astype(BF).astype(F32)
    larger = (jnp.maximum(counts[0], counts[1]) / length).astype(BF).astype(F32)
    rest = total - larger
    row = lax.broadcasted_iota(jnp.int32, (2 * LANES, 2 * LANES), 0)
    col = lax.broadcasted_iota(jnp.int32, (2 * LANES, 2 * LANES), 1)
    diagonal = (row == col) & (row % LANES < half)
    for parity in range(2):
        th, tl = ty_ref[parity, 0], ty_ref[parity, 1]
        keep = picked[parity]
        mh = (th.astype(F32) * keep).astype(BF)
        ml = (tl.astype(F32) * keep).astype(BF)
        table = dot_nt(mh, th) + dot_nt(ml, th) + dot_nt(mh, tl)
        value = jnp.where(counts[parity] >= counts[1 - parity], larger, rest)
        if parity:
            value = jnp.where(counts[1] > counts[0], larger, rest)
        h_ref[parity] = jnp.where(diagonal, value, table).astype(BF)


def make_wave(psf_ref, psft_ref, wave_ref, length, classes):
    half = length // 2
    readout = psf_ref.shape[1]
    blank = jnp.zeros((LANES - half, readout), F32)
    psf = jnp.concatenate([psf_ref[:half], blank, psf_ref[half:], blank], 0) * (0.5 / np.pi)
    wide = -(-readout // LANES) * LANES
    if wide > readout:
        psf = jnp.concatenate([psf, jnp.zeros((2 * LANES, wide - readout), F32)], 1)
    for side in range(2):
        psft_ref[side] = psf[side * LANES:(side + 1) * LANES].T
    rows = readout // classes
    for j in range(classes):
        picked = pl.ds(j, rows, stride=classes)
        c, s = turn_pair(jnp.concatenate([psft_ref[0, picked, :], psft_ref[1, picked, :]], 1))
        wave_ref[0, j] = c
        wave_ref[1, j] = s


def one_coil(coil, rot_ref, acc_ref, pt_ref, ct_ref, wave_ref, h_ref, w_ref, length, classes):
    width = rot_ref.shape[1]
    half = width // 2
    cr = spread(coil[0], length).astype(F32)
    ci = spread(coil[1], length).astype(F32)
    rr, ri = rot_ref[0], rot_ref[1]
    zr = cr * rr - ci * ri
    zi = cr * ri + ci * rr
    ar, ai, br, bi = zr[:half], zi[:half], zr[half:], zi[half:]
    for j in range(classes // 2):
        angle = -2 * np.pi * j / classes
        wr, wi = float(np.cos(angle)), float(np.sin(angle))
        if j == 0:
            ur, ui = br, bi
        else:
            ur, ui = br * wr - bi * wi, br * wi + bi * wr
        for step in range(2):
            cls = j + step * (classes // 2)
            tr, ti = (ar - ur, ai - ui) if step else (ar + ur, ai + ui)
            spectra = dot(pt_ref[cls], jnp.concatenate([tr, ti], 0).astype(BF))
            sr, si = spectra[:half], spectra[half:]
            c, s = wave_ref[0, cls], wave_ref[1, cls]
            vr = sr * c - si * s
            vi = sr * s + si * c
            rows = pl.ds(cls * half, half)
            w_ref[0, rows, :LANES] = (vr[:, :LANES] + vr[:, LANES:]).astype(BF)
            w_ref[0, rows, LANES:] = (vi[:, :LANES] + vi[:, LANES:]).astype(BF)
            w_ref[1, rows, :LANES] = (vr[:, :LANES] - vr[:, LANES:]).astype(BF)
            w_ref[1, rows, LANES:] = (vi[:, :LANES] - vi[:, LANES:]).astype(BF)
    back0 = back1 = None
    for j in range(classes // 2):
        pair = []
        for step in range(2):
            cls = j + step * (classes // 2)
            rows = pl.ds(cls * half, half)
            plus = dot(w_ref[0, rows, :], h_ref[0])
            minus = dot(w_ref[1, rows, :], h_ref[1])
            low, high = plus + minus, plus - minus
            yr = jnp.concatenate([low[:, :LANES], high[:, :LANES]], 1)
            yi = jnp.concatenate([low[:, LANES:], high[:, LANES:]], 1)
            c, s = wave_ref[0, cls], wave_ref[1, cls]
            ur = yr * c + yi * s
            ui = yi * c - yr * s
            pair.append(dot(ct_ref[cls], jnp.concatenate([ur, ui], 0).astype(BF)))
        total, diff = pair[0] + pair[1], pair[0] - pair[1]
        angle = 2 * np.pi * j / classes
        wr, wi = float(np.cos(angle)), float(np.sin(angle))
        dr, di = diff[:half], diff[half:]
        if j == 0:
            back0, back1 = total, [dr, di]
        else:
            back0 = back0 + total
            back1 = [back1[0] + (dr * wr - di * wi), back1[1] + (dr * wi + di * wr)]
    backr = jnp.concatenate([back0[:half], back1[0]], 0)
    backi = jnp.concatenate([back0[half:], back1[1]], 0)
    acc_ref[0] += cr * backr + ci * backi
    acc_ref[1] += cr * backi - ci * backr


def kernel(
    motion_ref, mask_ref, image_ref, psf_ref, coil_ref, pt_ref, ct_ref, tx_ref, ty_ref, out_ref,
    rot_ref, acc_ref, p1_ref, pc_ref, p3_ref, psft_ref, wave_ref, h_ref, w_ref, *, length, classes,
):
    step = pl.program_id(0)
    width = rot_ref.shape[1]
    half = length // 2

    @pl.when(step == 0)
    def _():
        make_phases(motion_ref, p1_ref, pc_ref, p3_ref, width, length)
        re, im = spread(image_ref[0], length), spread(image_ref[1], length)
        re, im = shear_rows(re, im, tx_ref, p1_ref, 1.0)
        re, im = shear_columns(re, im, ty_ref, pc_ref, 1.0)
        re, im = shear_rows(re, im, tx_ref, p3_ref, 1.0)
        rot_ref[0] = re
        rot_ref[1] = im
        acc_ref[...] = jnp.zeros_like(acc_ref)
        make_projector(mask_ref, ty_ref, h_ref, length)
        make_wave(psf_ref, psft_ref, wave_ref, length, classes)

    for c in range(coil_ref.shape[0]):
        one_coil(coil_ref[c], rot_ref, acc_ref, pt_ref, ct_ref, wave_ref, h_ref, w_ref.at[c], length, classes)

    @pl.when(step == pl.num_programs(0) - 1)
    def _():
        re, im = acc_ref[0], acc_ref[1]
        re, im = shear_rows(re, im, tx_ref, p3_ref, -1.0)
        re, im = shear_columns(re, im, ty_ref, pc_ref, -1.0)
        re, im = shear_rows(re, im, tx_ref, p1_ref, -1.0)
        for part, value in enumerate((re, im)):
            out_ref[part] = jnp.concatenate([value[:, :half], value[:, LANES:LANES + half]], 1)


def slice_operator(motion, mask, image, psf, coils):
    _, width, length = image.shape
    readout = psf.shape[1]
    count = coils.shape[0]
    classes = readout // (width // 2)
    pads, crops = readout_tables(width, readout)
    tx, ty = row_tables(width), column_tables(length)
    per_step = 2 if count % 2 == 0 else 1
    whole = lambda shape: pl.BlockSpec(shape, lambda i: (0,) * len(shape))
    wide = -(-readout // LANES) * LANES
    return pl.pallas_call(
        functools.partial(kernel, length=length, classes=classes),
        grid=(count // per_step,),
        in_specs=[
            pl.BlockSpec(memory_space=pltpu.SMEM),
            whole(mask.shape),
            whole(image.shape),
            whole(psf.shape),
            pl.BlockSpec((per_step, 2, width, length), lambda i: (i, 0, 0, 0)),
            whole(pads.shape),
            whole(crops.shape),
            whole(tx.shape),
            whole(ty.shape),
        ],
        out_specs=whole(image.shape),
        out_shape=jax.ShapeDtypeStruct(image.shape, F32),
        scratch_shapes=[
            pltpu.VMEM((2, width, 2 * LANES), F32),
            pltpu.VMEM((2, width, 2 * LANES), F32),
            pltpu.VMEM((2, width, 2 * LANES), F32),
            pltpu.VMEM((4, width, LANES), F32),
            pltpu.VMEM((2, width, 2 * LANES), F32),
            pltpu.VMEM((2, wide, LANES), F32),
            pltpu.VMEM((2, classes, width // 2, 2 * LANES), F32),
            pltpu.VMEM((2, 2 * LANES, 2 * LANES), BF),
            pltpu.VMEM((per_step, 2, readout, 2 * LANES), BF),
        ],
        compiler_params=pltpu.CompilerParams(vmem_limit_bytes=48 * 2**20),
        name="normal_operator",
    )(motion, mask, image, psf, coils, jnp.asarray(pads), jnp.asarray(crops), jnp.asarray(tx), jnp.asarray(ty))


def from_partner(value, axis, apart):
    mask = 2**apart
    pairs = [(source, source ^ mask) for source in range(lax.axis_size(axis))]
    return lax.ppermute(value, axis, pairs)


def gather_slice(values, bit_count, device_rank):
    for bit_index in range(bit_count):
        partner = from_partner(values, "space", bit_index)
        low_side = device_rank >> bit_index & 1 == 0
        values = jnp.where(
            low_side, jnp.concatenate([values, partner], 0), jnp.concatenate([partner, values], 0)
        )
    return values


def sum_slice(values, bit_count, device_rank):
    for bit_index in reversed(range(bit_count)):
        half_rows = values.shape[0] // 2
        low_side = device_rank >> bit_index & 1 == 0
        kept_part = jnp.where(low_side, values[:half_rows], values[half_rows:])
        sent_part = jnp.where(low_side, values[half_rows:], values[:half_rows])
        values = kept_part + from_partner(sent_part, "space", bit_index)
    return values


def regroup_coils(coil_maps, bit_count, device_rank):
    group_size = 1 << bit_count
    pieces = coil_maps.reshape((group_size, coil_maps.shape[0] // group_size) + coil_maps.shape[1:])
    for bit_index in range(bit_count):
        old_shape = pieces.shape
        halves = pieces.reshape((group_size >> bit_index + 1, 2, 1 << bit_index) + old_shape[1:])
        low_side = device_rank >> bit_index & 1 == 0
        kept_part = jnp.where(low_side, halves[:, 0], halves[:, 1])
        sent_part = jnp.where(low_side, halves[:, 1], halves[:, 0])
        partner = from_partner(sent_part, "space", bit_index)
        pieces = jnp.stack(
            [jnp.where(low_side, kept_part, partner), jnp.where(low_side, partner, kept_part)], 1
        ).reshape(old_shape)
    moved = jnp.moveaxis(pieces, 0, 1)
    return moved.reshape((moved.shape[0], group_size * coil_maps.shape[1]) + coil_maps.shape[2:])


def on_device(image, coil_maps, psf_phase, line_mask, motion):
    lines = image.shape[0]
    length = line_mask.shape[1]
    device_rank = lax.axis_index("space")
    group_size = max(1, length // lines)
    bit_count = group_size.bit_length() - 1
    if bit_count:
        coil_maps = regroup_coils(coil_maps, bit_count, device_rank)
        psf_phase = gather_slice(psf_phase, bit_count, device_rank)
        image = gather_slice(image, bit_count, device_rank)
    image = jnp.transpose(image, (1, 2, 0))
    coil_maps = jnp.transpose(coil_maps, (0, 2, 3, 1))
    results = []
    for start in range(0, image.shape[2], length):
        stop = start + length
        results.append(
            slice_operator(
                motion, line_mask, image[:, :, start:stop], psf_phase[start:stop], coil_maps[..., start:stop]
            )
        )
    result = results[0] if len(results) == 1 else jnp.concatenate(results, 2)
    if bit_count:
        result = jnp.transpose(result, (2, 0, 1))
        result = sum_slice(result, bit_count, device_rank)
        result = jnp.transpose(result, (1, 2, 0))
    shots = lax.axis_size("shot")
    total = result
    for apart in range(1, shots):
        pairs = [(source, (source + apart) % shots) for source in range(shots)]
        total = total + lax.ppermute(result, "shot", pairs)
    return jnp.transpose(total, (2, 0, 1))


def solution(mesh):
    in_specs = (
        P(("parts", "space"), None, None),
        P(None, ("parts", "space"), None, None),
        P(("parts", "space"), None),
        P(("parts", "shot"), None),
        P(("parts", "shot"), None),
    )
    out_specs = P(("parts", "space"), None, None)
    return jax.shard_map(
        on_device, mesh=mesh, in_specs=in_specs, out_specs=out_specs, check_vma=False
    )
```

```python
import functools

import jax
import jax.numpy as jnp
import numpy as np
from jax import lax
from jax.experimental import pallas as pl
from jax.experimental.pallas import tpu as pltpu
from jax.sharding import PartitionSpec as P

LEVELS = 17
ANGLE_STEP = 0.02
SHIFT_STEP = 0.5
LANES = 128
BF = jnp.bfloat16
F32 = jnp.float32


def split_pair(table):
    high = table.astype(np.float32).astype(BF)
    low = (table - high.astype(np.float64)).astype(np.float32).astype(BF)
    return np.stack([high, low])


def row_tables(width):
    index = np.arange(width)
    angle = 2 * np.pi * (np.outer(index, index) % width) / width
    return split_pair(np.concatenate([np.cos(angle), np.sin(angle)], 0) / np.sqrt(width))


def column_tables(length):
    half = length // 2
    result = []
    for parity in range(2):
        inputs = np.arange(half)[:, None]
        freqs = 2 * np.arange(half)[None, :] + parity
        angle = -2 * np.pi * (inputs * freqs % length) / length
        wave = np.exp(1j * angle) / np.sqrt(length)
        table = np.zeros((2 * LANES, 2 * LANES))
        table[:half, :half] = wave.real
        table[:half, LANES:LANES + half] = wave.imag
        table[LANES:LANES + half, :half] = -wave.imag
        table[LANES:LANES + half, LANES:LANES + half] = wave.real
        result.append(split_pair(table))
    return np.stack(result)


def readout_tables(width, readout):
    half = width // 2
    classes = readout // half
    pads, crops = [], []
    for j in range(classes):
        k = np.arange(half)[:, None] * classes + j
        x = np.arange(width)[None, :]
        angle = -2 * np.pi * (k * x % readout) / readout
        cosine = (np.cos(angle) / np.sqrt(readout)).astype(np.float32).astype(BF)
        sine = (np.sin(angle) / np.sqrt(readout)).astype(np.float32).astype(BF)
        pads.append(np.block([[cosine[:, :half], -sine[:, :half]], [sine[:, :half], cosine[:, :half]]]))
        crops.append(np.block([[cosine.T, sine.T], [-sine.T, cosine.T]]))
    return np.stack(pads), np.concatenate(crops, 1)


def turn_polys():
    nodes = np.cos(np.pi * (np.arange(400) + 0.5) / 400) * 0.125 + 0.125
    root = np.sqrt(nodes)
    out = []
    for value in (np.cos(2 * np.pi * root), np.sin(2 * np.pi * root) / root):
        series = np.polynomial.chebyshev.Chebyshev.fit(nodes, value, 6, domain=[0, 0.25])
        out.append([float(c) for c in series.convert(kind=np.polynomial.Polynomial).coef])
    return out


COS_POLY, SIN_POLY = turn_polys()


def turn_pair(turns):
    square = turns * turns
    cosine = jnp.full_like(square, COS_POLY[-1])
    sine = jnp.full_like(square, SIN_POLY[-1])
    for c, s in zip(COS_POLY[-2::-1], SIN_POLY[-2::-1]):
        cosine = cosine * square + c
        sine = sine * square + s
    return cosine, sine * turns


def wrap(turns):
    return turns - jnp.floor(turns + 0.5)


def dot(left, right):
    return jnp.dot(left, right, preferred_element_type=F32)


def dot_nt(left, right):
    return lax.dot_general(left, right, (((1,), (1,)), ((), ())), preferred_element_type=F32)


def two(value):
    high = value.astype(BF)
    return high, (value - high.astype(F32)).astype(BF)


def spread(value, length):
    half = length // 2
    blank = jnp.zeros((value.shape[0], LANES - half), value.dtype)
    return jnp.concatenate([value[:, :half], blank, value[:, half:], blank], 1)


def table_rows(tx_ref, value):
    high, low = two(value)
    return dot(tx_ref[0], high) + dot(tx_ref[1], high) + dot(tx_ref[0], low)


def shear_rows(re, im, tx_ref, phase_ref, sign):
    width = re.shape[0]
    from_re, from_im = table_rows(tx_ref, re), table_rows(tx_ref, im)
    sr = from_re[:width] + from_im[width:]
    si = from_im[:width] - from_re[width:]
    c, s = phase_ref[0, :width], phase_ref[1, :width] * sign
    from_re, from_im = table_rows(tx_ref, sr * c - si * s), table_rows(tx_ref, sr * s + si * c)
    return from_re[:width] - from_im[width:], from_im[:width] + from_re[width:]


def shear_columns(re, im, ty_ref, phase_ref, sign):
    width = re.shape[0]
    back = []
    for parity in range(2):
        join = (lambda v: v[:, :LANES] - v[:, LANES:]) if parity else (lambda v: v[:, :LANES] + v[:, LANES:])
        high, low = two(jnp.concatenate([join(re), join(im)], 1))
        th, tl = ty_ref[parity, 0], ty_ref[parity, 1]
        spectra = dot(high, th) + dot(low, th) + dot(high, tl)
        sr, si = spectra[:, :LANES], spectra[:, LANES:]
        c, s = phase_ref[parity, 0, :width], phase_ref[parity, 1, :width] * sign
        high, low = two(jnp.concatenate([sr * c - si * s, sr * s + si * c], 1))
        back.append(dot_nt(high, th) + dot_nt(low, th) + dot_nt(high, tl))
    even, odd = back
    low_half, high_half = even + odd, even - odd
    return (
        jnp.concatenate([low_half[:, :LANES], high_half[:, :LANES]], 1),
        jnp.concatenate([low_half[:, LANES:], high_half[:, LANES:]], 1),
    )


def signed(counter, length):
    return jnp.where(counter < length // 2, counter, counter - length).astype(F32)


def put(ref, re, im):
    ref[0, :re.shape[0]] = re
    ref[1, :im.shape[0]] = im


def make_phases(motion_ref, p1_ref, pc_ref, p3_ref, width, length):
    half = length // 2
    center = (LEVELS - 1) / 2.0
    shift_x = (motion_ref[0, 1].astype(F32) - center) * SHIFT_STEP
    shift_y = (motion_ref[0, 2].astype(F32) - center) * SHIFT_STEP
    angle = jnp.full((8, LANES), (motion_ref[0, 0].astype(F32) - center) * ANGLE_STEP, F32)
    tilt = jnp.sin(angle)[:1, :1]
    slope = -(jnp.sin(angle * 0.5) / jnp.cos(angle * 0.5))[:1, :1]
    lane = lax.broadcasted_iota(jnp.int32, (1, 2 * LANES), 1)
    line = jnp.where(lane < LANES, lane, lane - LANES + half)
    bend = slope * (line.astype(F32) - length / 2.0)
    freq = signed(lax.broadcasted_iota(jnp.int32, (width, 1), 0), width) * (-1.0 / width)
    c, s = turn_pair(wrap(freq * bend))
    put(p3_ref, c, s)
    cx, sx = turn_pair(wrap(freq * shift_x))
    put(p1_ref, c * cx - s * sx, c * sx + s * cx)
    along = lax.broadcasted_iota(jnp.int32, (width, 1), 0).astype(F32) - width / 2.0
    shift = tilt * along + shift_y
    lane = lax.broadcasted_iota(jnp.int32, (1, LANES), 1)
    for parity in range(2):
        freq = signed(2 * lane + parity, length) * (-1.0 / length)
        c, s = turn_pair(wrap(shift * freq))
        put(pc_ref.at[parity], c, s)


def make_projector(mask_ref, ty_ref, h_ref, length):
    half = length // 2
    mask = jnp.broadcast_to(mask_ref[...].astype(F32), (8, length)).astype(BF)
    line = lax.broadcasted_iota(jnp.int32, (length, 2 * LANES), 0)
    lane = lax.broadcasted_iota(jnp.int32, (length, 2 * LANES), 1) % LANES
    picked = []
    for parity in range(2):
        select = jnp.where((line == 2 * lane + parity) & (lane < half), 1.0, 0.0).astype(BF)
        picked.append(dot(mask, select)[:1])
    counts = [jnp.sum(p[:, :LANES], 1, keepdims=True) for p in picked]
    total = ((counts[0] + counts[1]) / length).astype(BF).astype(F32)
    larger = (jnp.maximum(counts[0], counts[1]) / length).astype(BF).astype(F32)
    rest = total - larger
    row = lax.broadcasted_iota(jnp.int32, (2 * LANES, 2 * LANES), 0)
    col = lax.broadcasted_iota(jnp.int32, (2 * LANES, 2 * LANES), 1)
    diagonal = (row == col) & (row % LANES < half)
    for parity in range(2):
        th, tl = ty_ref[parity, 0], ty_ref[parity, 1]
        keep = picked[parity]
        mh = (th.astype(F32) * keep).astype(BF)
        ml = (tl.astype(F32) * keep).astype(BF)
        table = dot_nt(mh, th) + dot_nt(ml, th) + dot_nt(mh, tl)
        value = jnp.where(counts[parity] >= counts[1 - parity], larger, rest)
        if parity:
            value = jnp.where(counts[1] > counts[0], larger, rest)
        h_ref[parity] = jnp.where(diagonal, value, table).astype(BF)


def make_wave(psf_ref, psft_ref, wave_ref, length, classes):
    half = length // 2
    readout = psf_ref.shape[1]
    blank = jnp.zeros((LANES - half, readout), F32)
    psf = jnp.concatenate([psf_ref[:half], blank, psf_ref[half:], blank], 0) * (0.5 / np.pi)
    wide = -(-readout // LANES) * LANES
    if wide > readout:
        psf = jnp.concatenate([psf, jnp.zeros((2 * LANES, wide - readout), F32)], 1)
    for side in range(2):
        psft_ref[side] = psf[side * LANES:(side + 1) * LANES].T
    rows = readout // classes
    for j in range(classes):
        picked = pl.ds(j, rows, stride=classes)
        c, s = turn_pair(jnp.concatenate([psft_ref[0, picked, :], psft_ref[1, picked, :]], 1))
        put(wave_ref.at[j], c.astype(BF), s.astype(BF))


def one_coil(coil, rot_ref, acc_ref, pt_ref, ct_ref, wave_ref, h_ref, w_ref, u_ref, length, classes):
    width = coil.shape[1]
    half = width // 2
    cr = spread(coil[0], length)
    ci = spread(coil[1], length)
    rr, ri = rot_ref[0, :width], rot_ref[1, :width]
    zr = (cr.astype(F32) * rr - ci.astype(F32) * ri).astype(BF)
    zi = (cr.astype(F32) * ri + ci.astype(F32) * rr).astype(BF)
    ar, ai, br, bi = zr[:half], zi[:half], zr[half:], zi[half:]
    for j in range(classes // 2):
        angle = -2 * np.pi * j / classes
        wr, wi = float(np.cos(angle)), float(np.sin(angle))
        if j == 0:
            ur, ui = br, bi
        else:
            ur, ui = br * wr - bi * wi, br * wi + bi * wr
        for step in range(2):
            cls = j + step * (classes // 2)
            tr, ti = (ar - ur, ai - ui) if step else (ar + ur, ai + ui)
            spectra = dot(pt_ref[cls], jnp.concatenate([tr, ti], 0)).astype(BF)
            sr, si = spectra[:half], spectra[half:]
            c, s = wave_ref[cls, 0, :half], wave_ref[cls, 1, :half]
            vr = sr * c - si * s
            vi = sr * s + si * c
            rows = pl.ds(cls * half, half)
            w_ref[0, rows, :LANES] = vr[:, :LANES] + vr[:, LANES:]
            w_ref[0, rows, LANES:] = vi[:, :LANES] + vi[:, LANES:]
            w_ref[1, rows, :LANES] = vr[:, :LANES] - vr[:, LANES:]
            w_ref[1, rows, LANES:] = vi[:, :LANES] - vi[:, LANES:]
    readout = classes * half
    plus = dot(w_ref[0, :readout], h_ref[0]).astype(BF)
    minus = dot(w_ref[1, :readout], h_ref[1]).astype(BF)
    for cls in range(classes):
        rows = slice(cls * half, (cls + 1) * half)
        for side, y in enumerate((plus[rows] + minus[rows], plus[rows] - minus[rows])):
            lanes = slice(side * LANES, (side + 1) * LANES)
            yr, yi = y[:, :LANES], y[:, LANES:]
            c, s = wave_ref[cls, 0, :half, lanes], wave_ref[cls, 1, :half, lanes]
            u_ref[pl.ds(2 * cls * half, half), lanes] = yr * c + yi * s
            u_ref[pl.ds((2 * cls + 1) * half, half), lanes] = yi * c - yr * s
    back = dot(ct_ref[...], u_ref[...])
    br, bi = back[:width], back[width:]
    crf, cif = cr.astype(F32), ci.astype(F32)
    acc_ref[0, :width] += crf * br + cif * bi
    acc_ref[1, :width] += crf * bi - cif * br


def kernel(
    motion_hbm, mask_hbm, image_hbm, tx_hbm, ty_hbm, psf_hbm, pt_hbm, coil_hbm, ct_hbm, out_ref,
    motion_ref, mask_ref, image_ref, tx_ref, ty_ref, psf_ref, pt_ref, coil_ref, ct_ref,
    rot_ref, acc_ref, p1_ref, pc_ref, p3_ref, psft_ref, wave_ref, h_ref, w_ref, u_ref, sems,
    *, length, classes, per_step,
):
    width = image_ref.shape[1]
    half = length // 2
    sources = (motion_hbm, mask_hbm, image_hbm, tx_hbm, ty_hbm, psf_hbm, pt_hbm, coil_hbm, ct_hbm)
    targets = (motion_ref, mask_ref, image_ref, tx_ref, ty_ref, psf_ref, pt_ref, coil_ref, ct_ref)
    copies = [pltpu.make_async_copy(a, b, sems.at[i]) for i, (a, b) in enumerate(zip(sources, targets))]
    for copy in copies:
        copy.start()
    for copy in copies[:6]:
        copy.wait()
    make_phases(motion_ref, p1_ref, pc_ref, p3_ref, width, length)
    re, im = spread(image_ref[0], length), spread(image_ref[1], length)
    re, im = shear_rows(re, im, tx_ref, p1_ref, 1.0)
    re, im = shear_columns(re, im, ty_ref, pc_ref, 1.0)
    re, im = shear_rows(re, im, tx_ref, p3_ref, 1.0)
    put(rot_ref, re, im)
    acc_ref[...] = jnp.zeros_like(acc_ref)
    make_projector(mask_ref, ty_ref, h_ref, length)
    make_wave(psf_ref, psft_ref, wave_ref, length, classes)
    for copy in copies[6:]:
        copy.wait()

    def some_coils(step, carry):
        for c in range(per_step):
            one_coil(
                coil_ref[step * per_step + c], rot_ref, acc_ref, pt_ref, ct_ref, wave_ref, h_ref,
                w_ref.at[c], u_ref.at[c], length, classes,
            )
        return carry

    lax.fori_loop(0, coil_ref.shape[0] // per_step, some_coils, 0)

    re, im = acc_ref[0, :width], acc_ref[1, :width]
    re, im = shear_rows(re, im, tx_ref, p3_ref, -1.0)
    re, im = shear_columns(re, im, ty_ref, pc_ref, -1.0)
    re, im = shear_rows(re, im, tx_ref, p1_ref, -1.0)
    for part, value in enumerate((re, im)):
        out_ref[part] = jnp.concatenate([value[:, :half], value[:, LANES:LANES + half]], 1)


def slice_operator(motion, mask, image, psf, coils):
    _, width, length = image.shape
    readout = psf.shape[1]
    count = coils.shape[0]
    classes = readout // (width // 2)
    pads, crops = readout_tables(width, readout)
    tx, ty = row_tables(width), column_tables(length)
    per_step = 2 if count % 2 == 0 else 1
    wide = -(-readout // LANES) * LANES
    operands = (motion, mask, image, jnp.asarray(tx), jnp.asarray(ty), psf, jnp.asarray(pads), coils, jnp.asarray(crops))
    return pl.pallas_call(
        functools.partial(kernel, length=length, classes=classes, per_step=per_step),
        in_specs=[pl.BlockSpec(memory_space=pltpu.HBM) for _ in operands],
        out_specs=pl.BlockSpec(memory_space=pltpu.VMEM),
        out_shape=jax.ShapeDtypeStruct(image.shape, F32),
        scratch_shapes=[pltpu.SMEM(motion.shape, motion.dtype)]
        + [pltpu.VMEM(a.shape, a.dtype) for a in operands[1:]]
        + [
            pltpu.VMEM((2, width + 8, 2 * LANES), F32),
            pltpu.VMEM((2, width + 8, 2 * LANES), F32),
            pltpu.VMEM((2, width + 8, 2 * LANES), F32),
            pltpu.VMEM((2, 2, width + 8, LANES), F32),
            pltpu.VMEM((2, width + 8, 2 * LANES), F32),
            pltpu.VMEM((2, wide, LANES), F32),
            pltpu.VMEM((classes, 2, width // 2 + 16, 2 * LANES), BF),
            pltpu.VMEM((2, 2 * LANES, 2 * LANES), BF),
            pltpu.VMEM((per_step, 2, readout + 16, 2 * LANES), BF),
            pltpu.VMEM((per_step, 2 * readout, 2 * LANES), BF),
            pltpu.SemaphoreType.DMA((len(operands),)),
        ],
        compiler_params=pltpu.CompilerParams(vmem_limit_bytes=64 * 2**20 - 2**16),
        name="normal_operator",
    )(*operands)


def from_partner(value, axis, apart):
    mask = 2**apart
    pairs = [(source, source ^ mask) for source in range(lax.axis_size(axis))]
    return lax.ppermute(value, axis, pairs)


def gather_slice(values, bit_count, device_rank):
    for bit_index in range(bit_count):
        partner = from_partner(values, "space", bit_index)
        low_side = device_rank >> bit_index & 1 == 0
        values = jnp.where(
            low_side, jnp.concatenate([values, partner], 0), jnp.concatenate([partner, values], 0)
        )
    return values


def sum_slice(values, bit_count, device_rank):
    for bit_index in reversed(range(bit_count)):
        half_rows = values.shape[0] // 2
        low_side = device_rank >> bit_index & 1 == 0
        kept_part = jnp.where(low_side, values[:half_rows], values[half_rows:])
        sent_part = jnp.where(low_side, values[half_rows:], values[:half_rows])
        values = kept_part + from_partner(sent_part, "space", bit_index)
    return values


def regroup_coils(coil_maps, bit_count, device_rank):
    group_size = 1 << bit_count
    pieces = coil_maps.reshape((group_size, coil_maps.shape[0] // group_size) + coil_maps.shape[1:])
    for bit_index in range(bit_count):
        old_shape = pieces.shape
        halves = pieces.reshape((group_size >> bit_index + 1, 2, 1 << bit_index) + old_shape[1:])
        low_side = device_rank >> bit_index & 1 == 0
        kept_part = jnp.where(low_side, halves[:, 0], halves[:, 1])
        sent_part = jnp.where(low_side, halves[:, 1], halves[:, 0])
        partner = from_partner(sent_part, "space", bit_index)
        pieces = jnp.stack(
            [jnp.where(low_side, kept_part, partner), jnp.where(low_side, partner, kept_part)], 1
        ).reshape(old_shape)
    moved = jnp.moveaxis(pieces, 0, 1)
    return moved.reshape((moved.shape[0], group_size * coil_maps.shape[1]) + coil_maps.shape[2:])


def on_device(image, coil_maps, psf_phase, line_mask, motion):
    lines = image.shape[0]
    length = line_mask.shape[1]
    device_rank = lax.axis_index("space")
    group_size = max(1, length // lines)
    bit_count = group_size.bit_length() - 1
    if bit_count:
        coil_maps = regroup_coils(coil_maps, bit_count, device_rank)
        psf_phase = gather_slice(psf_phase, bit_count, device_rank)
        image = gather_slice(image, bit_count, device_rank)
    image = jnp.transpose(image, (1, 2, 0))
    coil_maps = jnp.transpose(coil_maps, (0, 2, 3, 1))
    results = []
    for start in range(0, image.shape[2], length):
        stop = start + length
        results.append(
            slice_operator(
                motion, line_mask, image[:, :, start:stop], psf_phase[start:stop], coil_maps[..., start:stop]
            )
        )
    result = results[0] if len(results) == 1 else jnp.concatenate(results, 2)
    if bit_count:
        result = jnp.transpose(result, (2, 0, 1))
        result = sum_slice(result, bit_count, device_rank)
        result = jnp.transpose(result, (1, 2, 0))
    shots = lax.axis_size("shot")
    total = result
    for apart in range(1, shots):
        pairs = [(source, (source + apart) % shots) for source in range(shots)]
        total = total + lax.ppermute(result, "shot", pairs)
    return jnp.transpose(total, (2, 0, 1))


def solution(mesh):
    in_specs = (
        P(("parts", "space"), None, None),
        P(None, ("parts", "space"), None, None),
        P(("parts", "space"), None),
        P(("parts", "shot"), None),
        P(("parts", "shot"), None),
    )
    out_specs = P(("parts", "space"), None, None)
    return jax.shard_map(
        on_device, mesh=mesh, in_specs=in_specs, out_specs=out_specs, check_vma=False
    )
```

```python
import functools

import jax
import jax.numpy as jnp
import numpy as np
from jax import lax
from jax.experimental import pallas as pl
from jax.experimental.pallas import tpu as pltpu
from jax.sharding import PartitionSpec as P

LEVELS = 17
ANGLE_STEP = 0.02
SHIFT_STEP = 0.5
LANES = 128
UNROLL = 1
BF = jnp.bfloat16
F32 = jnp.float32


def split_pair(table):
    high = table.astype(np.float32).astype(BF)
    low = (table - high.astype(np.float64)).astype(np.float32).astype(BF)
    return np.stack([high, low])


def row_tables(width):
    half = width // 2
    result = []
    for parity in range(2):
        freqs = 2 * np.arange(half)[:, None] + parity
        wave = np.exp(-2j * np.pi * (freqs * np.arange(half)[None, :] % width) / width) / np.sqrt(width)
        table = np.block([[wave.real, -wave.imag], [wave.imag, wave.real]])
        result.append([split_pair(table), split_pair(table.T)])
    return np.array(result, BF)


def column_tables(length):
    half = length // 2
    result = []
    for parity in range(2):
        inputs = np.arange(half)[:, None]
        freqs = 2 * np.arange(half)[None, :] + parity
        angle = -2 * np.pi * (inputs * freqs % length) / length
        wave = np.exp(1j * angle) / np.sqrt(length)
        table = np.zeros((2 * LANES, 2 * LANES))
        table[:half, :half] = wave.real
        table[:half, LANES:LANES + half] = wave.imag
        table[LANES:LANES + half, :half] = -wave.imag
        table[LANES:LANES + half, LANES:LANES + half] = wave.real
        result.append(split_pair(table))
    return np.stack(result)


def readout_tables(width, readout):
    half = width // 2
    classes = readout // half
    pads, crops = [], []
    for j in range(classes):
        k = np.arange(half)[:, None] * classes + j
        x = np.arange(width)[None, :]
        angle = -2 * np.pi * (k * x % readout) / readout
        cosine = (np.cos(angle) / np.sqrt(readout)).astype(np.float32).astype(BF)
        sine = (np.sin(angle) / np.sqrt(readout)).astype(np.float32).astype(BF)
        pads.append(np.block([[cosine[:, :half], -sine[:, :half]], [sine[:, :half], cosine[:, :half]]]))
        crops.append(np.block([[cosine.T, sine.T], [-sine.T, cosine.T]]))
    return np.stack(pads), np.concatenate(crops, 1)


def turn_polys():
    nodes = np.cos(np.pi * (np.arange(400) + 0.5) / 400) * 0.125 + 0.125
    root = np.sqrt(nodes)
    out = []
    for value in (np.cos(2 * np.pi * root), np.sin(2 * np.pi * root) / root):
        series = np.polynomial.chebyshev.Chebyshev.fit(nodes, value, 6, domain=[0, 0.25])
        out.append([float(c) for c in series.convert(kind=np.polynomial.Polynomial).coef])
    return out


COS_POLY, SIN_POLY = turn_polys()


def turn_pair(turns):
    square = turns * turns
    cosine = jnp.full_like(square, COS_POLY[-1])
    sine = jnp.full_like(square, SIN_POLY[-1])
    for c, s in zip(COS_POLY[-2::-1], SIN_POLY[-2::-1]):
        cosine = cosine * square + c
        sine = sine * square + s
    return cosine, sine * turns


def wrap(turns):
    return turns - jnp.floor(turns + 0.5)


def dot(left, right):
    return jnp.dot(left, right, preferred_element_type=F32)


def dot_nt(left, right):
    return lax.dot_general(left, right, (((1,), (1,)), ((), ())), preferred_element_type=F32)


def two(value):
    high = value.astype(BF)
    return high, (value - high.astype(F32)).astype(BF)


def spread(value, length):
    half = length // 2
    blank = jnp.zeros((value.shape[0], LANES - half), value.dtype)
    return jnp.concatenate([value[:, :half], blank, value[:, half:], blank], 1)


def table_rows(tx_ref, parity, way, value):
    high, low = two(value)
    th, tl = tx_ref[parity, way, 0], tx_ref[parity, way, 1]
    return dot(th, high) + dot(tl, high) + dot(th, low)


def shear_rows(re, im, tx_ref, phase_ref, sign):
    half = re.shape[0] // 2
    back = []
    for parity in range(2):
        join = (lambda v: v[:half] - v[half:]) if parity else (lambda v: v[:half] + v[half:])
        spectra = table_rows(tx_ref, parity, 0, jnp.concatenate([join(re), join(im)], 0))
        sr, si = spectra[:half], spectra[half:]
        rows = slice(parity * half, (parity + 1) * half)
        c, s = phase_ref[0, rows], phase_ref[1, rows] * sign
        back.append(table_rows(tx_ref, parity, 1, jnp.concatenate([sr * c - si * s, sr * s + si * c], 0)))
    even, odd = back
    low, high = even + odd, even - odd
    return jnp.concatenate([low[:half], high[:half]], 0), jnp.concatenate([low[half:], high[half:]], 0)


def shear_columns(re, im, ty_ref, phase_ref, sign):
    width = re.shape[0]
    back = []
    for parity in range(2):
        join = (lambda v: v[:, :LANES] - v[:, LANES:]) if parity else (lambda v: v[:, :LANES] + v[:, LANES:])
        high, low = two(jnp.concatenate([join(re), join(im)], 1))
        th, tl = ty_ref[parity, 0], ty_ref[parity, 1]
        spectra = dot(high, th) + dot(low, th) + dot(high, tl)
        sr, si = spectra[:, :LANES], spectra[:, LANES:]
        c, s = phase_ref[parity, 0, :width], phase_ref[parity, 1, :width] * sign
        high, low = two(jnp.concatenate([sr * c - si * s, sr * s + si * c], 1))
        back.append(dot_nt(high, th) + dot_nt(low, th) + dot_nt(high, tl))
    even, odd = back
    low_half, high_half = even + odd, even - odd
    return (
        jnp.concatenate([low_half[:, :LANES], high_half[:, :LANES]], 1),
        jnp.concatenate([low_half[:, LANES:], high_half[:, LANES:]], 1),
    )


def signed(counter, length):
    return jnp.where(counter < length // 2, counter, counter - length).astype(F32)


def put(ref, re, im):
    ref[0, :re.shape[0]] = re
    ref[1, :im.shape[0]] = im


def make_phases(motion_ref, p1_ref, pc_ref, p3_ref, width, length):
    half = length // 2
    center = (LEVELS - 1) / 2.0
    shift_x = (motion_ref[0, 1].astype(F32) - center) * SHIFT_STEP
    shift_y = (motion_ref[0, 2].astype(F32) - center) * SHIFT_STEP
    angle = jnp.full((8, LANES), (motion_ref[0, 0].astype(F32) - center) * ANGLE_STEP, F32)
    tilt = jnp.sin(angle)[:1, :1]
    slope = -(jnp.sin(angle * 0.5) / jnp.cos(angle * 0.5))[:1, :1]
    lane = lax.broadcasted_iota(jnp.int32, (1, 2 * LANES), 1)
    line = jnp.where(lane < LANES, lane, lane - LANES + half)
    bend = slope * (line.astype(F32) - length / 2.0)
    row = lax.broadcasted_iota(jnp.int32, (width, 1), 0)
    freq = signed(jnp.where(row < width // 2, 2 * row, 2 * row + 1 - width), width) * (-1.0 / width)
    c, s = turn_pair(wrap(freq * bend))
    put(p3_ref, c, s)
    cx, sx = turn_pair(wrap(freq * shift_x))
    put(p1_ref, c * cx - s * sx, c * sx + s * cx)
    along = lax.broadcasted_iota(jnp.int32, (width, 1), 0).astype(F32) - width / 2.0
    shift = tilt * along + shift_y
    lane = lax.broadcasted_iota(jnp.int32, (1, LANES), 1)
    for parity in range(2):
        freq = signed(2 * lane + parity, length) * (-1.0 / length)
        c, s = turn_pair(wrap(shift * freq))
        put(pc_ref.at[parity], c, s)


def make_projector(mask_ref, ty_ref, h_ref, length):
    half = length // 2
    mask = jnp.broadcast_to(mask_ref[...].astype(F32), (8, length)).astype(BF)
    line = lax.broadcasted_iota(jnp.int32, (length, 2 * LANES), 0)
    lane = lax.broadcasted_iota(jnp.int32, (length, 2 * LANES), 1) % LANES
    picked = []
    for parity in range(2):
        select = jnp.where((line == 2 * lane + parity) & (lane < half), 1.0, 0.0).astype(BF)
        picked.append(dot(mask, select)[:1])
    counts = [jnp.sum(p[:, :LANES], 1, keepdims=True) for p in picked]
    total = ((counts[0] + counts[1]) / length).astype(BF).astype(F32)
    larger = (jnp.maximum(counts[0], counts[1]) / length).astype(BF).astype(F32)
    rest = total - larger
    row = lax.broadcasted_iota(jnp.int32, (2 * LANES, 2 * LANES), 0)
    col = lax.broadcasted_iota(jnp.int32, (2 * LANES, 2 * LANES), 1)
    diagonal = (row == col) & (row % LANES < half)
    for parity in range(2):
        th, tl = ty_ref[parity, 0], ty_ref[parity, 1]
        keep = picked[parity]
        mh = (th.astype(F32) * keep).astype(BF)
        ml = (tl.astype(F32) * keep).astype(BF)
        table = dot_nt(mh, th) + dot_nt(ml, th) + dot_nt(mh, tl)
        value = jnp.where(counts[parity] >= counts[1 - parity], larger, rest)
        if parity:
            value = jnp.where(counts[1] > counts[0], larger, rest)
        h_ref[parity] = jnp.where(diagonal, value, table).astype(BF)


def make_wave(psf_ref, psft_ref, wave_ref, length, classes):
    half = length // 2
    readout = psf_ref.shape[1]
    blank = jnp.zeros((LANES - half, readout), F32)
    psf = jnp.concatenate([psf_ref[:half], blank, psf_ref[half:], blank], 0) * (0.5 / np.pi)
    wide = -(-readout // LANES) * LANES
    if wide > readout:
        psf = jnp.concatenate([psf, jnp.zeros((2 * LANES, wide - readout), F32)], 1)
    for side in range(2):
        psft_ref[side] = psf[side * LANES:(side + 1) * LANES].T
    rows = readout // classes
    for j in range(classes):
        picked = pl.ds(j, rows, stride=classes)
        c, s = turn_pair(jnp.concatenate([psft_ref[0, picked, :], psft_ref[1, picked, :]], 1))
        put(wave_ref.at[j], c.astype(BF), s.astype(BF))


def encode(coil, rot_ref, pt_ref, wave_ref, c_ref, w_ref, length, classes):
    width = coil.shape[1]
    half = width // 2
    cr = spread(coil[0], length)
    ci = spread(coil[1], length)
    put(c_ref, cr, ci)
    rr, ri = rot_ref[0, :width], rot_ref[1, :width]
    zr = (cr.astype(F32) * rr - ci.astype(F32) * ri).astype(BF)
    zi = (cr.astype(F32) * ri + ci.astype(F32) * rr).astype(BF)
    ar, ai, br, bi = zr[:half], zi[:half], zr[half:], zi[half:]
    for j in range(classes // 2):
        angle = -2 * np.pi * j / classes
        wr, wi = float(np.cos(angle)), float(np.sin(angle))
        if j == 0:
            ur, ui = br, bi
        else:
            ur, ui = br * wr - bi * wi, br * wi + bi * wr
        for step in range(2):
            cls = j + step * (classes // 2)
            tr, ti = (ar - ur, ai - ui) if step else (ar + ur, ai + ui)
            spectra = dot(pt_ref[cls], jnp.concatenate([tr, ti], 0)).astype(BF)
            sr, si = spectra[:half], spectra[half:]
            c, s = wave_ref[cls, 0, :half], wave_ref[cls, 1, :half]
            vr = sr * c - si * s
            vi = sr * s + si * c
            rows = pl.ds(cls * half, half)
            w_ref[0, rows, :LANES] = vr[:, :LANES] + vr[:, LANES:]
            w_ref[0, rows, LANES:] = vi[:, :LANES] + vi[:, LANES:]
            w_ref[1, rows, :LANES] = vr[:, :LANES] - vr[:, LANES:]
            w_ref[1, rows, LANES:] = vi[:, :LANES] - vi[:, LANES:]


def project(wave_ref, h_ref, w_ref, u_ref, half, classes):
    readout = classes * half
    plus = dot(w_ref[0, :readout], h_ref[0]).astype(BF)
    minus = dot(w_ref[1, :readout], h_ref[1]).astype(BF)
    for cls in range(classes):
        rows = slice(cls * half, (cls + 1) * half)
        for side, y in enumerate((plus[rows] + minus[rows], plus[rows] - minus[rows])):
            lanes = slice(side * LANES, (side + 1) * LANES)
            yr, yi = y[:, :LANES], y[:, LANES:]
            c, s = wave_ref[cls, 0, :half, lanes], wave_ref[cls, 1, :half, lanes]
            u_ref[pl.ds(2 * cls * half, half), lanes] = yr * c + yi * s
            u_ref[pl.ds((2 * cls + 1) * half, half), lanes] = yi * c - yr * s


def decode(acc_ref, ct_ref, c_ref, u_ref, width):
    back = dot(ct_ref[...], u_ref[...])
    br, bi = back[:width], back[width:]
    cr, ci = c_ref[0, :width].astype(F32), c_ref[1, :width].astype(F32)
    acc_ref[0, :width] += cr * br + ci * bi
    acc_ref[1, :width] += cr * bi - ci * br


def kernel(
    motion_hbm, mask_hbm, image_hbm, tx_hbm, ty_hbm, psf_hbm, pt_hbm, coil_hbm, ct_hbm, out_ref,
    motion_ref, mask_ref, image_ref, tx_ref, ty_ref, psf_ref, pt_ref, coil_ref, ct_ref,
    rot_ref, acc_ref, p1_ref, pc_ref, p3_ref, psft_ref, wave_ref, h_ref, c_ref, w_ref, u_ref, sems,
    *, length, classes, unroll,
):
    width = image_ref.shape[1]
    half = length // 2
    sources = (motion_hbm, mask_hbm, image_hbm, tx_hbm, ty_hbm, psf_hbm, pt_hbm, coil_hbm, ct_hbm)
    targets = (motion_ref, mask_ref, image_ref, tx_ref, ty_ref, psf_ref, pt_ref, coil_ref, ct_ref)
    copies = [pltpu.make_async_copy(a, b, sems.at[i]) for i, (a, b) in enumerate(zip(sources, targets))]
    for copy in copies[:6]:
        copy.start()
    for copy in copies[:4]:
        copy.wait()
    for copy in copies[6:]:
        copy.start()
    for copy in copies[4:6]:
        copy.wait()
    make_phases(motion_ref, p1_ref, pc_ref, p3_ref, width, length)
    re, im = spread(image_ref[0], length), spread(image_ref[1], length)
    re, im = shear_rows(re, im, tx_ref, p1_ref, 1.0)
    re, im = shear_columns(re, im, ty_ref, pc_ref, 1.0)
    re, im = shear_rows(re, im, tx_ref, p3_ref, 1.0)
    put(rot_ref, re, im)
    acc_ref[...] = jnp.zeros_like(acc_ref)
    make_projector(mask_ref, ty_ref, h_ref, length)
    make_wave(psf_ref, psft_ref, wave_ref, length, classes)
    for copy in copies[6:]:
        copy.wait()

    count = coil_ref.shape[0]

    def run(stage, coil):
        slot = coil % 2 if isinstance(coil, int) else coil[1]
        index = coil if isinstance(coil, int) else coil[0]
        if stage == 0:
            encode(coil_ref[index], rot_ref, pt_ref, wave_ref, c_ref.at[slot], w_ref.at[slot], length, classes)
        elif stage == 1:
            project(wave_ref, h_ref, w_ref.at[slot], u_ref.at[slot], width // 2, classes)
        else:
            decode(acc_ref, ct_ref, c_ref.at[slot], u_ref.at[slot], width)

    def pair(first):
        run(2, (first - 2, 0))
        run(1, (first - 1, 1))
        run(0, (first, 0))
        run(2, (first - 1, 1))
        run(1, (first, 0))
        run(0, (first + 1, 1))

    if count % 2:
        def single(coil, carry):
            for stage in range(3):
                run(stage, (coil, 0))
            return carry

        lax.fori_loop(0, count, single, 0)
    else:
        pairs = count // 2 - 1
        run(0, 0)
        run(1, 0)
        run(0, 1)
        steps = pairs // unroll
        for extra in range(pairs - steps * unroll):
            pair(2 * extra + 2)

        def some_pairs(step, carry):
            for inner in range(unroll):
                pair(2 * (pairs - steps * unroll + step * unroll + inner) + 2)
            return carry

        if steps:
            lax.fori_loop(0, steps, some_pairs, 0)
        run(2, count - 2)
        run(1, count - 1)
        run(2, count - 1)

    re, im = acc_ref[0, :width], acc_ref[1, :width]
    re, im = shear_rows(re, im, tx_ref, p3_ref, -1.0)
    re, im = shear_columns(re, im, ty_ref, pc_ref, -1.0)
    re, im = shear_rows(re, im, tx_ref, p1_ref, -1.0)
    for part, value in enumerate((re, im)):
        out_ref[part] = jnp.concatenate([value[:, :half], value[:, LANES:LANES + half]], 1)


def slice_operator(motion, mask, image, psf, coils):
    _, width, length = image.shape
    readout = psf.shape[1]
    classes = readout // (width // 2)
    pads, crops = readout_tables(width, readout)
    tx, ty = row_tables(width), column_tables(length)
    wide = -(-readout // LANES) * LANES
    operands = (motion, mask, image, jnp.asarray(tx), jnp.asarray(ty), psf, jnp.asarray(pads), coils, jnp.asarray(crops))
    return pl.pallas_call(
        functools.partial(kernel, length=length, classes=classes, unroll=UNROLL),
        in_specs=[pl.BlockSpec(memory_space=pltpu.HBM) for _ in operands],
        out_specs=pl.BlockSpec(memory_space=pltpu.VMEM),
        out_shape=jax.ShapeDtypeStruct(image.shape, F32),
        scratch_shapes=[pltpu.SMEM(motion.shape, motion.dtype)]
        + [pltpu.VMEM(a.shape, a.dtype) for a in operands[1:]]
        + [
            pltpu.VMEM((2, width + 8, 2 * LANES), F32),
            pltpu.VMEM((2, width + 8, 2 * LANES), F32),
            pltpu.VMEM((2, width + 8, 2 * LANES), F32),
            pltpu.VMEM((2, 2, width + 8, LANES), F32),
            pltpu.VMEM((2, width + 8, 2 * LANES), F32),
            pltpu.VMEM((2, wide, LANES), F32),
            pltpu.VMEM((classes, 2, width // 2 + 16, 2 * LANES), BF),
            pltpu.VMEM((2, 2 * LANES, 2 * LANES), BF),
            pltpu.VMEM((2, 2, width + 16, 2 * LANES), BF),
            pltpu.VMEM((2, 2, readout + 16, 2 * LANES), BF),
            pltpu.VMEM((2, 2 * readout, 2 * LANES), BF),
            pltpu.SemaphoreType.DMA((len(operands),)),
        ],
        compiler_params=pltpu.CompilerParams(vmem_limit_bytes=40 * 2**20),
        name="normal_operator",
    )(*[pltpu.with_memory_space_constraint(a, pltpu.HBM) for a in operands])


def from_partner(value, axis, apart):
    mask = 2**apart
    pairs = [(source, source ^ mask) for source in range(lax.axis_size(axis))]
    return lax.ppermute(value, axis, pairs)


def gather_slice(values, bit_count, device_rank):
    for bit_index in range(bit_count):
        partner = from_partner(values, "space", bit_index)
        low_side = device_rank >> bit_index & 1 == 0
        values = jnp.where(
            low_side, jnp.concatenate([values, partner], 0), jnp.concatenate([partner, values], 0)
        )
    return values


def sum_slice(values, bit_count, device_rank):
    for bit_index in reversed(range(bit_count)):
        half_rows = values.shape[0] // 2
        low_side = device_rank >> bit_index & 1 == 0
        kept_part = jnp.where(low_side, values[:half_rows], values[half_rows:])
        sent_part = jnp.where(low_side, values[half_rows:], values[:half_rows])
        values = kept_part + from_partner(sent_part, "space", bit_index)
    return values


def regroup_coils(coil_maps, bit_count, device_rank):
    group_size = 1 << bit_count
    pieces = coil_maps.reshape((group_size, coil_maps.shape[0] // group_size) + coil_maps.shape[1:])
    for bit_index in range(bit_count):
        old_shape = pieces.shape
        halves = pieces.reshape((group_size >> bit_index + 1, 2, 1 << bit_index) + old_shape[1:])
        low_side = device_rank >> bit_index & 1 == 0
        kept_part = jnp.where(low_side, halves[:, 0], halves[:, 1])
        sent_part = jnp.where(low_side, halves[:, 1], halves[:, 0])
        partner = from_partner(sent_part, "space", bit_index)
        pieces = jnp.stack(
            [jnp.where(low_side, kept_part, partner), jnp.where(low_side, partner, kept_part)], 1
        ).reshape(old_shape)
    moved = jnp.moveaxis(pieces, 0, 1)
    return moved.reshape((moved.shape[0], group_size * coil_maps.shape[1]) + coil_maps.shape[2:])


def on_device(image, coil_maps, psf_phase, line_mask, motion):
    lines = image.shape[0]
    length = line_mask.shape[1]
    device_rank = lax.axis_index("space")
    group_size = max(1, length // lines)
    bit_count = group_size.bit_length() - 1
    if bit_count:
        coil_maps = regroup_coils(coil_maps, bit_count, device_rank)
        psf_phase = gather_slice(psf_phase, bit_count, device_rank)
        image = gather_slice(image, bit_count, device_rank)
    image = jnp.transpose(image, (1, 2, 0))
    coil_maps = jnp.transpose(coil_maps, (0, 2, 3, 1))
    results = []
    for start in range(0, image.shape[2], length):
        stop = start + length
        results.append(
            slice_operator(
                motion, line_mask, image[:, :, start:stop], psf_phase[start:stop], coil_maps[..., start:stop]
            )
        )
    result = results[0] if len(results) == 1 else jnp.concatenate(results, 2)
    if bit_count:
        result = jnp.transpose(result, (2, 0, 1))
        result = sum_slice(result, bit_count, device_rank)
        result = jnp.transpose(result, (1, 2, 0))
    shots = lax.axis_size("shot")
    total = result
    for apart in range(1, shots):
        pairs = [(source, (source + apart) % shots) for source in range(shots)]
        total = total + lax.ppermute(result, "shot", pairs)
    return jnp.transpose(total, (2, 0, 1))


def solution(mesh):
    in_specs = (
        P(("parts", "space"), None, None),
        P(None, ("parts", "space"), None, None),
        P(("parts", "space"), None),
        P(("parts", "shot"), None),
        P(("parts", "shot"), None),
    )
    out_specs = P(("parts", "space"), None, None)
    return jax.shard_map(
        on_device, mesh=mesh, in_specs=in_specs, out_specs=out_specs, check_vma=False
    )
```

```python
import functools

import jax
import jax.numpy as jnp
import numpy as np
from jax import lax
from jax.experimental import pallas as pl
from jax.experimental.pallas import tpu as pltpu
from jax.sharding import PartitionSpec as P

LEVELS = 17
ANGLE_STEP = 0.02
SHIFT_STEP = 0.5
LANES = 128
UNROLL = 7
BF = jnp.bfloat16
F32 = jnp.float32


def split_pair(table):
    high = table.astype(np.float32).astype(BF)
    low = (table - high.astype(np.float64)).astype(np.float32).astype(BF)
    return np.stack([high, low])


def row_tables(width):
    half = width // 2
    result = []
    for parity in range(2):
        freqs = 2 * np.arange(half)[:, None] + parity
        wave = np.exp(-2j * np.pi * (freqs * np.arange(half)[None, :] % width) / width) / np.sqrt(width)
        table = np.block([[wave.real, -wave.imag], [wave.imag, wave.real]])
        result.append(split_pair(table))
    return np.stack(result)


def column_tables(length):
    half = length // 2
    result = []
    for parity in range(2):
        inputs = np.arange(half)[:, None]
        freqs = 2 * np.arange(half)[None, :] + parity
        angle = -2 * np.pi * (inputs * freqs % length) / length
        wave = np.exp(1j * angle) / np.sqrt(length)
        table = np.zeros((2 * LANES, 2 * LANES))
        table[:half, :half] = wave.real
        table[:half, LANES:LANES + half] = wave.imag
        table[LANES:LANES + half, :half] = -wave.imag
        table[LANES:LANES + half, LANES:LANES + half] = wave.real
        result.append(split_pair(table))
    return np.stack(result)


def readout_tables(width, readout):
    half = width // 2
    classes = readout // half
    pads = []
    for j in range(classes):
        k = np.arange(half)[:, None] * classes + j
        x = np.arange(half)[None, :]
        angle = -2 * np.pi * (k * x % readout) / readout
        cosine = (np.cos(angle) / np.sqrt(readout)).astype(np.float32).astype(BF)
        sine = (np.sin(angle) / np.sqrt(readout)).astype(np.float32).astype(BF)
        pads.append(np.block([[cosine, -sine], [sine, cosine]]))
    return np.stack(pads)


def turn_polys():
    nodes = np.cos(np.pi * (np.arange(400) + 0.5) / 400) * 0.125 + 0.125
    root = np.sqrt(nodes)
    out = []
    for value in (np.cos(2 * np.pi * root), np.sin(2 * np.pi * root) / root):
        series = np.polynomial.chebyshev.Chebyshev.fit(nodes, value, 6, domain=[0, 0.25])
        out.append([float(c) for c in series.convert(kind=np.polynomial.Polynomial).coef])
    return out


COS_POLY, SIN_POLY = turn_polys()


def turn_pair(turns):
    square = turns * turns
    cosine = jnp.full_like(square, COS_POLY[-1])
    sine = jnp.full_like(square, SIN_POLY[-1])
    for c, s in zip(COS_POLY[-2::-1], SIN_POLY[-2::-1]):
        cosine = cosine * square + c
        sine = sine * square + s
    return cosine, sine * turns


def wrap(turns):
    return turns - jnp.floor(turns + 0.5)


def dot(left, right):
    return jnp.dot(left, right, preferred_element_type=F32)


def dot_nt(left, right):
    return lax.dot_general(left, right, (((1,), (1,)), ((), ())), preferred_element_type=F32)


def two(value):
    high = value.astype(BF)
    return high, (value - high.astype(F32)).astype(BF)


def spread(value, length):
    half = length // 2
    blank = jnp.zeros((value.shape[0], LANES - half), value.dtype)
    return jnp.concatenate([value[:, :half], blank, value[:, half:], blank], 1)


def table_rows(table_ref, value):
    high, low = two(value)
    th, tl = table_ref[0], table_ref[1]
    return dot(th, high) + dot(tl, high) + dot(th, low)


def shear_rows(re, im, tx_ref, txt_ref, phase_ref, sign):
    half = re.shape[0] // 2
    back = []
    for parity in range(2):
        join = (lambda v: v[:half] - v[half:]) if parity else (lambda v: v[:half] + v[half:])
        spectra = table_rows(tx_ref.at[parity], jnp.concatenate([join(re), join(im)], 0))
        sr, si = spectra[:half], spectra[half:]
        rows = slice(parity * half, (parity + 1) * half)
        c, s = phase_ref[0, rows], phase_ref[1, rows] * sign
        back.append(table_rows(txt_ref.at[parity], jnp.concatenate([sr * c - si * s, sr * s + si * c], 0)))
    even, odd = back
    low, high = even + odd, even - odd
    return jnp.concatenate([low[:half], high[:half]], 0), jnp.concatenate([low[half:], high[half:]], 0)


def shear_columns(re, im, ty_ref, phase_ref, sign):
    width = re.shape[0]
    back = []
    for parity in range(2):
        join = (lambda v: v[:, :LANES] - v[:, LANES:]) if parity else (lambda v: v[:, :LANES] + v[:, LANES:])
        high, low = two(jnp.concatenate([join(re), join(im)], 1))
        th, tl = ty_ref[parity, 0], ty_ref[parity, 1]
        spectra = dot(high, th) + dot(low, th) + dot(high, tl)
        sr, si = spectra[:, :LANES], spectra[:, LANES:]
        c, s = phase_ref[parity, 0, :width], phase_ref[parity, 1, :width] * sign
        high, low = two(jnp.concatenate([sr * c - si * s, sr * s + si * c], 1))
        back.append(dot_nt(high, th) + dot_nt(low, th) + dot_nt(high, tl))
    even, odd = back
    low_half, high_half = even + odd, even - odd
    return (
        jnp.concatenate([low_half[:, :LANES], high_half[:, :LANES]], 1),
        jnp.concatenate([low_half[:, LANES:], high_half[:, LANES:]], 1),
    )


def signed(counter, length):
    return jnp.where(counter < length // 2, counter, counter - length).astype(F32)


def put(ref, re, im):
    ref[0, :re.shape[0]] = re
    ref[1, :im.shape[0]] = im


def make_phases(motion_ref, p1_ref, pc_ref, p3_ref, width, length):
    half = length // 2
    center = (LEVELS - 1) / 2.0
    shift_x = (motion_ref[0, 1].astype(F32) - center) * SHIFT_STEP
    shift_y = (motion_ref[0, 2].astype(F32) - center) * SHIFT_STEP
    angle = jnp.full((8, LANES), (motion_ref[0, 0].astype(F32) - center) * ANGLE_STEP, F32)
    tilt = jnp.sin(angle)[:1, :1]
    slope = -(jnp.sin(angle * 0.5) / jnp.cos(angle * 0.5))[:1, :1]
    lane = lax.broadcasted_iota(jnp.int32, (1, 2 * LANES), 1)
    line = jnp.where(lane < LANES, lane, lane - LANES + half)
    bend = slope * (line.astype(F32) - length / 2.0)
    row = lax.broadcasted_iota(jnp.int32, (width, 1), 0)
    freq = signed(jnp.where(row < width // 2, 2 * row, 2 * row + 1 - width), width) * (-1.0 / width)
    c, s = turn_pair(wrap(freq * bend))
    put(p3_ref, c, s)
    cx, sx = turn_pair(wrap(freq * shift_x))
    put(p1_ref, c * cx - s * sx, c * sx + s * cx)
    along = lax.broadcasted_iota(jnp.int32, (width, 1), 0).astype(F32) - width / 2.0
    shift = tilt * along + shift_y
    lane = lax.broadcasted_iota(jnp.int32, (1, LANES), 1)
    for parity in range(2):
        freq = signed(2 * lane + parity, length) * (-1.0 / length)
        c, s = turn_pair(wrap(shift * freq))
        put(pc_ref.at[parity], c, s)


def make_projector(mask_ref, ty_ref, h_ref, length):
    half = length // 2
    mask = jnp.broadcast_to(mask_ref[...].astype(F32), (8, length)).astype(BF)
    line = lax.broadcasted_iota(jnp.int32, (length, 2 * LANES), 0)
    lane = lax.broadcasted_iota(jnp.int32, (length, 2 * LANES), 1) % LANES
    picked = []
    for parity in range(2):
        select = jnp.where((line == 2 * lane + parity) & (lane < half), 1.0, 0.0).astype(BF)
        picked.append(dot(mask, select)[:1])
    counts = [jnp.sum(p[:, :LANES], 1, keepdims=True) for p in picked]
    total = ((counts[0] + counts[1]) / length).astype(BF).astype(F32)
    larger = (jnp.maximum(counts[0], counts[1]) / length).astype(BF).astype(F32)
    rest = total - larger
    row = lax.broadcasted_iota(jnp.int32, (2 * LANES, 2 * LANES), 0)
    col = lax.broadcasted_iota(jnp.int32, (2 * LANES, 2 * LANES), 1)
    diagonal = (row == col) & (row % LANES < half)
    for parity in range(2):
        th, tl = ty_ref[parity, 0], ty_ref[parity, 1]
        keep = picked[parity]
        mh = (th.astype(F32) * keep).astype(BF)
        ml = (tl.astype(F32) * keep).astype(BF)
        table = dot_nt(mh, th) + dot_nt(ml, th) + dot_nt(mh, tl)
        value = jnp.where(counts[parity] >= counts[1 - parity], larger, rest)
        if parity:
            value = jnp.where(counts[1] > counts[0], larger, rest)
        h_ref[parity] = jnp.where(diagonal, value, table).astype(BF)


def make_wave(psf_ref, psft_ref, wave_ref, length, classes):
    half = length // 2
    readout = psf_ref.shape[1]
    blank = jnp.zeros((LANES - half, readout), F32)
    psf = jnp.concatenate([psf_ref[:half], blank, psf_ref[half:], blank], 0) * (0.5 / np.pi)
    wide = -(-readout // LANES) * LANES
    if wide > readout:
        psf = jnp.concatenate([psf, jnp.zeros((2 * LANES, wide - readout), F32)], 1)
    for side in range(2):
        psft_ref[side] = psf[side * LANES:(side + 1) * LANES].T
    rows = readout // classes
    for j in range(classes):
        picked = pl.ds(j, rows, stride=classes)
        c, s = turn_pair(jnp.concatenate([psft_ref[0, picked, :], psft_ref[1, picked, :]], 1))
        put(wave_ref.at[j], c.astype(BF), s.astype(BF))


def make_inverse_rows(tx_ref, txt_ref):
    for parity in range(2):
        for part in range(2):
            txt_ref[parity, part] = tx_ref[parity, part].astype(F32).T.astype(BF)


def make_crop(pt_ref, ct_ref, half, classes):
    for j in range(classes):
        back = pt_ref[j].astype(F32).T
        re, im = back[:half], back[half:]
        angle = 2 * np.pi * j / classes
        wr, wi = float(np.cos(angle)), float(np.sin(angle))
        columns = pl.ds(2 * half * j, 2 * half)
        ct_ref[pl.ds(0, half), columns] = re.astype(BF)
        ct_ref[pl.ds(half, half), columns] = (re * wr - im * wi).astype(BF)
        ct_ref[pl.ds(2 * half, half), columns] = im.astype(BF)
        ct_ref[pl.ds(3 * half, half), columns] = (re * wi + im * wr).astype(BF)


def encode(coil, rot_ref, pt_ref, wave_ref, c_ref, w_ref, length, classes):
    width = coil.shape[1]
    half = width // 2
    cr = spread(coil[0], length)
    ci = spread(coil[1], length)
    put(c_ref, cr, ci)
    rr, ri = rot_ref[0, :width], rot_ref[1, :width]
    zr = (cr.astype(F32) * rr - ci.astype(F32) * ri).astype(BF)
    zi = (cr.astype(F32) * ri + ci.astype(F32) * rr).astype(BF)
    ar, ai, br, bi = zr[:half], zi[:half], zr[half:], zi[half:]
    for j in range(classes // 2):
        angle = -2 * np.pi * j / classes
        wr, wi = float(np.cos(angle)), float(np.sin(angle))
        if j == 0:
            ur, ui = br, bi
        else:
            ur, ui = br * wr - bi * wi, br * wi + bi * wr
        for step in range(2):
            cls = j + step * (classes // 2)
            tr, ti = (ar - ur, ai - ui) if step else (ar + ur, ai + ui)
            spectra = dot(pt_ref[cls], jnp.concatenate([tr, ti], 0)).astype(BF)
            sr, si = spectra[:half], spectra[half:]
            c, s = wave_ref[cls, 0, :half], wave_ref[cls, 1, :half]
            vr = sr * c - si * s
            vi = sr * s + si * c
            rows = pl.ds(cls * half, half)
            w_ref[0, rows, :LANES] = vr[:, :LANES] + vr[:, LANES:]
            w_ref[0, rows, LANES:] = vi[:, :LANES] + vi[:, LANES:]
            w_ref[1, rows, :LANES] = vr[:, :LANES] - vr[:, LANES:]
            w_ref[1, rows, LANES:] = vi[:, :LANES] - vi[:, LANES:]


def project(wave_ref, h_ref, w_ref, u_ref, half, classes):
    readout = classes * half
    plus = dot(w_ref[0, :readout], h_ref[0]).astype(BF)
    minus = dot(w_ref[1, :readout], h_ref[1]).astype(BF)
    for cls in range(classes):
        rows = slice(cls * half, (cls + 1) * half)
        for side, y in enumerate((plus[rows] + minus[rows], plus[rows] - minus[rows])):
            lanes = slice(side * LANES, (side + 1) * LANES)
            yr, yi = y[:, :LANES], y[:, LANES:]
            c, s = wave_ref[cls, 0, :half, lanes], wave_ref[cls, 1, :half, lanes]
            u_ref[pl.ds(2 * cls * half, half), lanes] = yr * c + yi * s
            u_ref[pl.ds((2 * cls + 1) * half, half), lanes] = yi * c - yr * s


def decode(acc_ref, ct_ref, c_ref, u_ref, width):
    back = dot(ct_ref[...], u_ref[...])
    br, bi = back[:width], back[width:]
    cr, ci = c_ref[0, :width].astype(F32), c_ref[1, :width].astype(F32)
    acc_ref[0, :width] += cr * br + ci * bi
    acc_ref[1, :width] += cr * bi - ci * br


def kernel(
    motion_hbm, mask_hbm, image_hbm, tx_hbm, ty_hbm, psf_hbm, pt_hbm, coil_hbm, out_ref,
    motion_ref, mask_ref, image_ref, tx_ref, ty_ref, psf_ref, pt_ref, coil_ref,
    txt_ref, ct_ref, rot_ref, acc_ref, p1_ref, pc_ref, p3_ref, psft_ref, wave_ref, h_ref, c_ref, w_ref, u_ref, sems,
    *, length, classes, unroll,
):
    width = image_ref.shape[1]
    half = length // 2
    sources = (motion_hbm, mask_hbm, image_hbm, tx_hbm, ty_hbm, psf_hbm, pt_hbm)
    targets = (motion_ref, mask_ref, image_ref, tx_ref, ty_ref, psf_ref, pt_ref)
    copies = [pltpu.make_async_copy(a, b, sems.at[i]) for i, (a, b) in enumerate(zip(sources, targets))]
    count = coil_ref.shape[0]
    chunk = 2 - count % 2

    def coil_copy(index):
        part = pl.ds(index * chunk, chunk)
        return pltpu.make_async_copy(coil_hbm.at[part], coil_ref.at[part], sems.at[len(sources) + index])

    for copy in copies:
        copy.start()
    copies[0].wait()
    make_phases(motion_ref, p1_ref, pc_ref, p3_ref, width, length)
    for copy in copies[1:4]:
        copy.wait()
    for index in range(count // chunk):
        coil_copy(index).start()
    make_inverse_rows(tx_ref, txt_ref)
    re, im = spread(image_ref[0], length), spread(image_ref[1], length)
    re, im = shear_rows(re, im, tx_ref, txt_ref, p1_ref, 1.0)
    acc_ref[...] = jnp.zeros_like(acc_ref)
    for copy in copies[4:]:
        copy.wait()
    make_crop(pt_ref, ct_ref, width // 2, classes)
    make_projector(mask_ref, ty_ref, h_ref, length)
    make_wave(psf_ref, psft_ref, wave_ref, length, classes)
    re, im = shear_columns(re, im, ty_ref, pc_ref, 1.0)
    re, im = shear_rows(re, im, tx_ref, txt_ref, p3_ref, 1.0)
    put(rot_ref, re, im)
    for index in range(count // chunk):
        coil_copy(index).wait()

    def run(stage, coil):
        slot = coil % 2 if isinstance(coil, int) else coil[1]
        index = coil if isinstance(coil, int) else coil[0]
        if stage == 0:
            encode(coil_ref[index], rot_ref, pt_ref, wave_ref, c_ref.at[slot], w_ref.at[slot], length, classes)
        elif stage == 1:
            project(wave_ref, h_ref, w_ref.at[slot], u_ref.at[slot], width // 2, classes)
        else:
            decode(acc_ref, ct_ref, c_ref.at[slot], u_ref.at[slot], width)

    def pair(first):
        run(2, (first - 2, 0))
        run(1, (first - 1, 1))
        run(0, (first, 0))
        run(2, (first - 1, 1))
        run(1, (first, 0))
        run(0, (first + 1, 1))

    if count % 2:
        def single(coil, carry):
            for stage in range(3):
                run(stage, (coil, 0))
            return carry

        lax.fori_loop(0, count, single, 0)
    else:
        pairs = count // 2 - 1
        run(0, 0)
        run(1, 0)
        run(0, 1)
        steps = pairs // unroll
        for extra in range(pairs - steps * unroll):
            pair(2 * extra + 2)

        def some_pairs(step, carry):
            for inner in range(unroll):
                pair(2 * (pairs - steps * unroll + step * unroll + inner) + 2)
            return carry

        if steps:
            lax.fori_loop(0, steps, some_pairs, 0)
        run(2, count - 2)
        run(1, count - 1)
        run(2, count - 1)

    re, im = acc_ref[0, :width], acc_ref[1, :width]
    re, im = shear_rows(re, im, tx_ref, txt_ref, p3_ref, -1.0)
    re, im = shear_columns(re, im, ty_ref, pc_ref, -1.0)
    re, im = shear_rows(re, im, tx_ref, txt_ref, p1_ref, -1.0)
    for part, value in enumerate((re, im)):
        out_ref[part] = jnp.concatenate([value[:, :half], value[:, LANES:LANES + half]], 1)


def slice_operator(motion, mask, image, psf, coils):
    _, width, length = image.shape
    readout = psf.shape[1]
    classes = readout // (width // 2)
    pads = readout_tables(width, readout)
    tx, ty = row_tables(width), column_tables(length)
    wide = -(-readout // LANES) * LANES
    operands = (motion, mask, image, jnp.asarray(tx), jnp.asarray(ty), psf, jnp.asarray(pads), coils)
    return pl.pallas_call(
        functools.partial(kernel, length=length, classes=classes, unroll=UNROLL),
        in_specs=[pl.BlockSpec(memory_space=pltpu.HBM) for _ in operands],
        out_specs=pl.BlockSpec(memory_space=pltpu.VMEM),
        out_shape=jax.ShapeDtypeStruct(image.shape, F32),
        scratch_shapes=[pltpu.SMEM(motion.shape, motion.dtype)]
        + [pltpu.VMEM(a.shape, a.dtype) for a in operands[1:]]
        + [
            pltpu.VMEM(tx.shape, BF),
            pltpu.VMEM((2 * width, classes * width), BF),
            pltpu.VMEM((2, width + 8, 2 * LANES), F32),
            pltpu.VMEM((2, width + 8, 2 * LANES), F32),
            pltpu.VMEM((2, width + 8, 2 * LANES), F32),
            pltpu.VMEM((2, 2, width + 8, LANES), F32),
            pltpu.VMEM((2, width + 8, 2 * LANES), F32),
            pltpu.VMEM((2, wide, LANES), F32),
            pltpu.VMEM((classes, 2, width // 2 + 16, 2 * LANES), BF),
            pltpu.VMEM((2, 2 * LANES, 2 * LANES), BF),
            pltpu.VMEM((2, 2, width + 16, 2 * LANES), BF),
            pltpu.VMEM((2, 2, readout + 16, 2 * LANES), BF),
            pltpu.VMEM((2, 2 * readout, 2 * LANES), BF),
            pltpu.SemaphoreType.DMA((len(operands) + coils.shape[0],)),
        ],
        compiler_params=pltpu.CompilerParams(vmem_limit_bytes=40 * 2**20),
        name="normal_operator",
    )(*[pltpu.with_memory_space_constraint(a, pltpu.HBM) for a in operands])


def from_partner(value, axis, apart):
    mask = 2**apart
    pairs = [(source, source ^ mask) for source in range(lax.axis_size(axis))]
    return lax.ppermute(value, axis, pairs)


def gather_slice(values, bit_count, device_rank):
    for bit_index in range(bit_count):
        partner = from_partner(values, "space", bit_index)
        low_side = device_rank >> bit_index & 1 == 0
        values = jnp.where(
            low_side, jnp.concatenate([values, partner], 0), jnp.concatenate([partner, values], 0)
        )
    return values


def sum_slice(values, bit_count, device_rank):
    for bit_index in reversed(range(bit_count)):
        half_rows = values.shape[0] // 2
        low_side = device_rank >> bit_index & 1 == 0
        kept_part = jnp.where(low_side, values[:half_rows], values[half_rows:])
        sent_part = jnp.where(low_side, values[half_rows:], values[:half_rows])
        values = kept_part + from_partner(sent_part, "space", bit_index)
    return values


def regroup_coils(coil_maps, bit_count, device_rank):
    group_size = 1 << bit_count
    pieces = coil_maps.reshape((group_size, coil_maps.shape[0] // group_size) + coil_maps.shape[1:])
    for bit_index in range(bit_count):
        old_shape = pieces.shape
        halves = pieces.reshape((group_size >> bit_index + 1, 2, 1 << bit_index) + old_shape[1:])
        low_side = device_rank >> bit_index & 1 == 0
        kept_part = jnp.where(low_side, halves[:, 0], halves[:, 1])
        sent_part = jnp.where(low_side, halves[:, 1], halves[:, 0])
        partner = from_partner(sent_part, "space", bit_index)
        pieces = jnp.stack(
            [jnp.where(low_side, kept_part, partner), jnp.where(low_side, partner, kept_part)], 1
        ).reshape(old_shape)
    moved = jnp.moveaxis(pieces, 0, 1)
    return moved.reshape((moved.shape[0], group_size * coil_maps.shape[1]) + coil_maps.shape[2:])


def on_device(image, coil_maps, psf_phase, line_mask, motion):
    lines = image.shape[0]
    length = line_mask.shape[1]
    device_rank = lax.axis_index("space")
    group_size = max(1, length // lines)
    bit_count = group_size.bit_length() - 1
    if bit_count:
        coil_maps = regroup_coils(coil_maps, bit_count, device_rank)
        psf_phase = gather_slice(psf_phase, bit_count, device_rank)
        image = gather_slice(image, bit_count, device_rank)
    image = jnp.transpose(image, (1, 2, 0))
    coil_maps = jnp.transpose(coil_maps, (0, 2, 3, 1))
    results = []
    for start in range(0, image.shape[2], length):
        stop = start + length
        results.append(
            slice_operator(
                motion, line_mask, image[:, :, start:stop], psf_phase[start:stop], coil_maps[..., start:stop]
            )
        )
    result = results[0] if len(results) == 1 else jnp.concatenate(results, 2)
    if bit_count:
        result = jnp.transpose(result, (2, 0, 1))
        result = sum_slice(result, bit_count, device_rank)
        result = jnp.transpose(result, (1, 2, 0))
    shots = lax.axis_size("shot")
    total = result
    for apart in range(1, shots):
        pairs = [(source, (source + apart) % shots) for source in range(shots)]
        total = total + lax.ppermute(result, "shot", pairs)
    return jnp.transpose(total, (2, 0, 1))


def solution(mesh):
    in_specs = (
        P(("parts", "space"), None, None),
        P(None, ("parts", "space"), None, None),
        P(("parts", "space"), None),
        P(("parts", "shot"), None),
        P(("parts", "shot"), None),
    )
    out_specs = P(("parts", "space"), None, None)
    return jax.shard_map(
        on_device, mesh=mesh, in_specs=in_specs, out_specs=out_specs, check_vma=False
    )
```

```python
import functools

import jax
import jax.numpy as jnp
import numpy as np
from jax import lax
from jax.experimental import pallas as pl
from jax.experimental.pallas import tpu as pltpu
from jax.sharding import PartitionSpec as P

LEVELS = 17
ANGLE_STEP = 0.02
SHIFT_STEP = 0.5
LANES = 128
UNROLL = 7
BF = jnp.bfloat16
F32 = jnp.float32


def split_pair(table):
    high = table.astype(np.float32).astype(BF)
    low = (table - high.astype(np.float64)).astype(np.float32).astype(BF)
    return np.stack([high, low])


def row_tables(width):
    half = width // 2
    result = []
    for parity in range(2):
        freqs = 2 * np.arange(half)[:, None] + parity
        wave = np.exp(-2j * np.pi * (freqs * np.arange(half)[None, :] % width) / width) / np.sqrt(width)
        table = np.block([[wave.real, -wave.imag], [wave.imag, wave.real]])
        result.append(split_pair(table))
    return np.stack(result)


def column_tables(length):
    half = length // 2
    result = []
    for parity in range(2):
        inputs = np.arange(half)[:, None]
        freqs = 2 * np.arange(half)[None, :] + parity
        angle = -2 * np.pi * (inputs * freqs % length) / length
        wave = np.exp(1j * angle) / np.sqrt(length)
        table = np.zeros((2 * LANES, 2 * LANES))
        table[:half, :half] = wave.real
        table[:half, LANES:LANES + half] = wave.imag
        table[LANES:LANES + half, :half] = -wave.imag
        table[LANES:LANES + half, LANES:LANES + half] = wave.real
        result.append(split_pair(table))
    return np.stack(result)


def readout_tables(width, readout):
    half = width // 2
    classes = readout // half
    pads = []
    for j in range(classes):
        k = np.arange(half)[:, None] * classes + j
        x = np.arange(half)[None, :]
        angle = -2 * np.pi * (k * x % readout) / readout
        cosine = (np.cos(angle) / np.sqrt(readout)).astype(np.float32).astype(BF)
        sine = (np.sin(angle) / np.sqrt(readout)).astype(np.float32).astype(BF)
        pads.append(np.block([[cosine, -sine], [sine, cosine]]))
    return np.stack(pads)


def turn_polys(degree):
    nodes = np.cos(np.pi * (np.arange(400) + 0.5) / 400) * 0.125 + 0.125
    root = np.sqrt(nodes)
    out = []
    for value in (np.cos(2 * np.pi * root), np.sin(2 * np.pi * root) / root):
        series = np.polynomial.chebyshev.Chebyshev.fit(nodes, value, degree, domain=[0, 0.25])
        out.append([float(c) for c in series.convert(kind=np.polynomial.Polynomial).coef])
    return out


FULL_POLY, WAVE_POLY = turn_polys(6), turn_polys(5)


def turn_pair(turns, poly=FULL_POLY):
    cos_poly, sin_poly = poly
    square = turns * turns
    cosine = jnp.full_like(square, cos_poly[-1])
    sine = jnp.full_like(square, sin_poly[-1])
    for c, s in zip(cos_poly[-2::-1], sin_poly[-2::-1]):
        cosine = cosine * square + c
        sine = sine * square + s
    return cosine, sine * turns


def wrap(turns):
    return turns - jnp.floor(turns + 0.5)


def dot(left, right):
    return jnp.dot(left, right, preferred_element_type=F32)


def dot_nt(left, right):
    return lax.dot_general(left, right, (((1,), (1,)), ((), ())), preferred_element_type=F32)


def two(value):
    high = value.astype(BF)
    return high, (value - high.astype(F32)).astype(BF)


def spread(value, length):
    half = length // 2
    blank = jnp.zeros((value.shape[0], LANES - half), value.dtype)
    return jnp.concatenate([value[:, :half], blank, value[:, half:], blank], 1)


def table_rows(table_ref, value):
    high, low = two(value)
    th, tl = table_ref[0], table_ref[1]
    return dot(th, high) + dot(tl, high) + dot(th, low)


def shear_rows(re, im, tx_ref, txt_ref, phase_ref, sign):
    half = re.shape[0] // 2
    back = []
    for parity in range(2):
        join = (lambda v: v[:half] - v[half:]) if parity else (lambda v: v[:half] + v[half:])
        spectra = table_rows(tx_ref.at[parity], jnp.concatenate([join(re), join(im)], 0))
        sr, si = spectra[:half], spectra[half:]
        rows = slice(parity * half, (parity + 1) * half)
        c, s = phase_ref[0, rows], phase_ref[1, rows] * sign
        back.append(table_rows(txt_ref.at[parity], jnp.concatenate([sr * c - si * s, sr * s + si * c], 0)))
    even, odd = back
    low, high = even + odd, even - odd
    return jnp.concatenate([low[:half], high[:half]], 0), jnp.concatenate([low[half:], high[half:]], 0)


def shear_columns(re, im, ty_ref, phase_ref, sign):
    width = re.shape[0]
    back = []
    for parity in range(2):
        join = (lambda v: v[:, :LANES] - v[:, LANES:]) if parity else (lambda v: v[:, :LANES] + v[:, LANES:])
        high, low = two(jnp.concatenate([join(re), join(im)], 1))
        th, tl = ty_ref[parity, 0], ty_ref[parity, 1]
        spectra = dot(high, th) + dot(low, th) + dot(high, tl)
        sr, si = spectra[:, :LANES], spectra[:, LANES:]
        c, s = phase_ref[parity, 0, :width], phase_ref[parity, 1, :width] * sign
        high, low = two(jnp.concatenate([sr * c - si * s, sr * s + si * c], 1))
        back.append(dot_nt(high, th) + dot_nt(low, th) + dot_nt(high, tl))
    even, odd = back
    low_half, high_half = even + odd, even - odd
    return (
        jnp.concatenate([low_half[:, :LANES], high_half[:, :LANES]], 1),
        jnp.concatenate([low_half[:, LANES:], high_half[:, LANES:]], 1),
    )


def signed(counter, length):
    return jnp.where(counter < length // 2, counter, counter - length).astype(F32)


def put(ref, re, im):
    ref[0, :re.shape[0]] = re
    ref[1, :im.shape[0]] = im


def make_phases(motion_ref, p1_ref, pc_ref, p3_ref, width, length):
    half = length // 2
    center = (LEVELS - 1) / 2.0
    shift_x = (motion_ref[0, 1].astype(F32) - center) * SHIFT_STEP
    shift_y = (motion_ref[0, 2].astype(F32) - center) * SHIFT_STEP
    angle = jnp.full((8, LANES), (motion_ref[0, 0].astype(F32) - center) * ANGLE_STEP, F32)
    tilt = jnp.sin(angle)[:1, :1]
    slope = -(jnp.sin(angle * 0.5) / jnp.cos(angle * 0.5))[:1, :1]
    lane = lax.broadcasted_iota(jnp.int32, (1, 2 * LANES), 1)
    line = jnp.where(lane < LANES, lane, lane - LANES + half)
    bend = slope * (line.astype(F32) - length / 2.0)
    side = width // 2
    coarse = signed(16 * lax.broadcasted_iota(jnp.int32, (-(-side // 64) * 8, 1), 0), width) * (-1.0 / width)
    fine = (2 * lax.broadcasted_iota(jnp.int32, (8, 1), 0)).astype(F32)
    for ref, shift in ((p1_ref, bend + shift_x), (p3_ref, bend)):
        gc, gs = turn_pair(wrap(coarse * shift))
        for parity in range(2):
            c, s = turn_pair(wrap((fine + parity) * (-1.0 / width) * shift))
            for a in range(side // 8):
                rows = pl.ds(parity * side + 8 * a, 8)
                ac, as_ = gc[a:a + 1], gs[a:a + 1]
                ref[0, rows] = c * ac - s * as_
                ref[1, rows] = c * as_ + s * ac
    lane = lax.broadcasted_iota(jnp.int32, (1, LANES), 1)
    coarse = (8 * lax.broadcasted_iota(jnp.int32, (-(-width // 64) * 8, 1), 0)).astype(F32) - width / 2.0
    fine = lax.broadcasted_iota(jnp.int32, (8, 1), 0).astype(F32)
    for parity in range(2):
        freq = signed(2 * lane + parity, length) * (-1.0 / length)
        gc, gs = turn_pair(wrap((tilt * coarse + shift_y) * freq))
        c, s = turn_pair(wrap(tilt * fine * freq))
        for a in range(width // 8):
            rows = pl.ds(8 * a, 8)
            ac, as_ = gc[a:a + 1], gs[a:a + 1]
            pc_ref[parity, 0, rows] = c * ac - s * as_
            pc_ref[parity, 1, rows] = c * as_ + s * ac


def make_projector(mask_ref, ty_ref, h_ref, length):
    half = length // 2
    mask = jnp.broadcast_to(mask_ref[...].astype(F32), (8, length)).astype(BF)
    line = lax.broadcasted_iota(jnp.int32, (length, 2 * LANES), 0)
    lane = lax.broadcasted_iota(jnp.int32, (length, 2 * LANES), 1) % LANES
    picked = []
    for parity in range(2):
        select = jnp.where((line == 2 * lane + parity) & (lane < half), 1.0, 0.0).astype(BF)
        picked.append(dot(mask, select)[:1])
    counts = [jnp.sum(p[:, :LANES], 1, keepdims=True) for p in picked]
    total = ((counts[0] + counts[1]) / length).astype(BF).astype(F32)
    larger = (jnp.maximum(counts[0], counts[1]) / length).astype(BF).astype(F32)
    rest = total - larger
    row = lax.broadcasted_iota(jnp.int32, (2 * LANES, 2 * LANES), 0)
    col = lax.broadcasted_iota(jnp.int32, (2 * LANES, 2 * LANES), 1)
    diagonal = (row == col) & (row % LANES < half)
    for parity in range(2):
        th, tl = ty_ref[parity, 0], ty_ref[parity, 1]
        keep = picked[parity]
        mh = (th.astype(F32) * keep).astype(BF)
        ml = (tl.astype(F32) * keep).astype(BF)
        table = dot_nt(mh, th) + dot_nt(ml, th) + dot_nt(mh, tl)
        value = jnp.where(counts[parity] >= counts[1 - parity], larger, rest)
        if parity:
            value = jnp.where(counts[1] > counts[0], larger, rest)
        h_ref[parity] = jnp.where(diagonal, value, table).astype(BF)


def make_wave(psf_ref, psft_ref, wave_ref, length, classes):
    half = length // 2
    readout = psf_ref.shape[1]
    blank = jnp.zeros((LANES - half, readout), F32)
    psf = jnp.concatenate([psf_ref[:half], blank, psf_ref[half:], blank], 0) * (0.5 / np.pi)
    wide = -(-readout // LANES) * LANES
    if wide > readout:
        psf = jnp.concatenate([psf, jnp.zeros((2 * LANES, wide - readout), F32)], 1)
    for side in range(2):
        psft_ref[side] = psf[side * LANES:(side + 1) * LANES].T
    rows = readout // classes
    for j in range(classes):
        picked = pl.ds(j, rows, stride=classes)
        c, s = turn_pair(jnp.concatenate([psft_ref[0, picked, :], psft_ref[1, picked, :]], 1), WAVE_POLY)
        put(wave_ref.at[j], c.astype(BF), s.astype(BF))


def make_inverse_rows(tx_ref, txt_ref):
    for parity in range(2):
        for part in range(2):
            txt_ref[parity, part] = tx_ref[parity, part].astype(F32).T.astype(BF)


def make_crop(pt_ref, ct_ref, half, classes):
    for j in range(classes):
        back = pt_ref[j].astype(F32).T
        re, im = back[:half], back[half:]
        angle = 2 * np.pi * j / classes
        wr, wi = float(np.cos(angle)), float(np.sin(angle))
        columns = pl.ds(2 * half * j, 2 * half)
        ct_ref[pl.ds(0, half), columns] = re.astype(BF)
        ct_ref[pl.ds(half, half), columns] = (re * wr - im * wi).astype(BF)
        ct_ref[pl.ds(2 * half, half), columns] = im.astype(BF)
        ct_ref[pl.ds(3 * half, half), columns] = (re * wi + im * wr).astype(BF)


def encode(coil, rot_ref, pt_ref, wave_ref, c_ref, w_ref, length, classes):
    width = coil.shape[1]
    half = width // 2
    cr = spread(coil[0], length)
    ci = spread(coil[1], length)
    put(c_ref, cr, ci)
    rr, ri = rot_ref[0, :width], rot_ref[1, :width]
    zr = (cr.astype(F32) * rr - ci.astype(F32) * ri).astype(BF)
    zi = (cr.astype(F32) * ri + ci.astype(F32) * rr).astype(BF)
    ar, ai, br, bi = zr[:half], zi[:half], zr[half:], zi[half:]
    for j in range(classes // 2):
        angle = -2 * np.pi * j / classes
        wr, wi = float(np.cos(angle)), float(np.sin(angle))
        if j == 0:
            ur, ui = br, bi
        else:
            ur, ui = br * wr - bi * wi, br * wi + bi * wr
        for step in range(2):
            cls = j + step * (classes // 2)
            tr, ti = (ar - ur, ai - ui) if step else (ar + ur, ai + ui)
            spectra = dot(pt_ref[cls], jnp.concatenate([tr, ti], 0)).astype(BF)
            sr, si = spectra[:half], spectra[half:]
            c, s = wave_ref[cls, 0, :half], wave_ref[cls, 1, :half]
            vr = sr * c - si * s
            vi = sr * s + si * c
            rows = pl.ds(cls * half, half)
            w_ref[0, rows, :LANES] = vr[:, :LANES] + vr[:, LANES:]
            w_ref[0, rows, LANES:] = vi[:, :LANES] + vi[:, LANES:]
            w_ref[1, rows, :LANES] = vr[:, :LANES] - vr[:, LANES:]
            w_ref[1, rows, LANES:] = vi[:, :LANES] - vi[:, LANES:]


def project(wave_ref, h_ref, w_ref, u_ref, half, classes):
    readout = classes * half
    plus = dot(w_ref[0, :readout], h_ref[0]).astype(BF)
    minus = dot(w_ref[1, :readout], h_ref[1]).astype(BF)
    for cls in range(classes):
        rows = slice(cls * half, (cls + 1) * half)
        for side, y in enumerate((plus[rows] + minus[rows], plus[rows] - minus[rows])):
            lanes = slice(side * LANES, (side + 1) * LANES)
            yr, yi = y[:, :LANES], y[:, LANES:]
            c, s = wave_ref[cls, 0, :half, lanes], wave_ref[cls, 1, :half, lanes]
            u_ref[pl.ds(2 * cls * half, half), lanes] = yr * c + yi * s
            u_ref[pl.ds((2 * cls + 1) * half, half), lanes] = yi * c - yr * s


def decode(acc_ref, ct_ref, c_ref, u_ref, width):
    back = dot(ct_ref[...], u_ref[...])
    br, bi = back[:width].astype(BF), back[width:].astype(BF)
    cr, ci = c_ref[0, :width], c_ref[1, :width]
    acc_ref[0, :width] += (cr * br + ci * bi).astype(F32)
    acc_ref[1, :width] += (cr * bi - ci * br).astype(F32)


def kernel(
    motion_hbm, mask_hbm, image_hbm, tx_hbm, ty_hbm, psf_hbm, pt_hbm, coil_hbm, out_ref,
    motion_ref, mask_ref, image_ref, tx_ref, ty_ref, psf_ref, pt_ref, coil_ref,
    txt_ref, ct_ref, rot_ref, acc_ref, p1_ref, pc_ref, p3_ref, psft_ref, wave_ref, h_ref, c_ref, w_ref, u_ref, sems,
    *, length, classes, unroll,
):
    width = image_ref.shape[1]
    half = length // 2
    sources = (motion_hbm, mask_hbm, image_hbm, tx_hbm, ty_hbm, psf_hbm, pt_hbm)
    targets = (motion_ref, mask_ref, image_ref, tx_ref, ty_ref, psf_ref, pt_ref)
    copies = [pltpu.make_async_copy(a, b, sems.at[i]) for i, (a, b) in enumerate(zip(sources, targets))]
    count = coil_ref.shape[0]
    chunk = 2 - count % 2

    def coil_copy(index):
        part = pl.ds(index * chunk, chunk)
        return pltpu.make_async_copy(coil_hbm.at[part], coil_ref.at[part], sems.at[len(sources) + index])

    for copy in copies:
        copy.start()
    copies[0].wait()
    make_phases(motion_ref, p1_ref, pc_ref, p3_ref, width, length)
    for copy in copies[1:4]:
        copy.wait()
    for index in range(count // chunk):
        coil_copy(index).start()
    make_inverse_rows(tx_ref, txt_ref)
    re, im = spread(image_ref[0], length), spread(image_ref[1], length)
    re, im = shear_rows(re, im, tx_ref, txt_ref, p1_ref, 1.0)
    acc_ref[...] = jnp.zeros_like(acc_ref)
    for copy in copies[4:]:
        copy.wait()
    make_crop(pt_ref, ct_ref, width // 2, classes)
    make_projector(mask_ref, ty_ref, h_ref, length)
    re, im = shear_columns(re, im, ty_ref, pc_ref, 1.0)
    re, im = shear_rows(re, im, tx_ref, txt_ref, p3_ref, 1.0)
    make_wave(psf_ref, psft_ref, wave_ref, length, classes)
    put(rot_ref, re, im)
    for index in range(count // chunk):
        coil_copy(index).wait()

    def run(stage, coil):
        slot = coil % 2 if isinstance(coil, int) else coil[1]
        index = coil if isinstance(coil, int) else coil[0]
        if stage == 0:
            encode(coil_ref[index], rot_ref, pt_ref, wave_ref, c_ref.at[slot], w_ref.at[slot], length, classes)
        elif stage == 1:
            project(wave_ref, h_ref, w_ref.at[slot], u_ref.at[slot], width // 2, classes)
        else:
            decode(acc_ref, ct_ref, c_ref.at[slot], u_ref.at[slot], width)

    def pair(first):
        run(2, (first - 2, 0))
        run(1, (first - 1, 1))
        run(0, (first, 0))
        run(2, (first - 1, 1))
        run(1, (first, 0))
        run(0, (first + 1, 1))

    if count % 2:
        def single(coil, carry):
            for stage in range(3):
                run(stage, (coil, 0))
            return carry

        lax.fori_loop(0, count, single, 0)
    else:
        pairs = count // 2 - 1
        run(0, 0)
        run(1, 0)
        run(0, 1)
        steps = pairs // unroll
        for extra in range(pairs - steps * unroll):
            pair(2 * extra + 2)

        def some_pairs(step, carry):
            for inner in range(unroll):
                pair(2 * (pairs - steps * unroll + step * unroll + inner) + 2)
            return carry

        if steps:
            lax.fori_loop(0, steps, some_pairs, 0)
        run(2, count - 2)
        run(1, count - 1)
        run(2, count - 1)

    re, im = acc_ref[0, :width], acc_ref[1, :width]
    re, im = shear_rows(re, im, tx_ref, txt_ref, p3_ref, -1.0)
    re, im = shear_columns(re, im, ty_ref, pc_ref, -1.0)
    re, im = shear_rows(re, im, tx_ref, txt_ref, p1_ref, -1.0)
    for part, value in enumerate((re, im)):
        out_ref[part] = jnp.concatenate([value[:, :half], value[:, LANES:LANES + half]], 1)


def slice_operator(motion, mask, image, psf, coils):
    _, width, length = image.shape
    readout = psf.shape[1]
    classes = readout // (width // 2)
    pads = readout_tables(width, readout)
    tx, ty = row_tables(width), column_tables(length)
    wide = -(-readout // LANES) * LANES
    operands = (motion, mask, image, jnp.asarray(tx), jnp.asarray(ty), psf, jnp.asarray(pads), coils)
    return pl.pallas_call(
        functools.partial(kernel, length=length, classes=classes, unroll=UNROLL),
        in_specs=[pl.BlockSpec(memory_space=pltpu.HBM) for _ in operands],
        out_specs=pl.BlockSpec(memory_space=pltpu.VMEM),
        out_shape=jax.ShapeDtypeStruct(image.shape, F32),
        scratch_shapes=[pltpu.SMEM(motion.shape, motion.dtype)]
        + [pltpu.VMEM(a.shape, a.dtype) for a in operands[1:]]
        + [
            pltpu.VMEM(tx.shape, BF),
            pltpu.VMEM((2 * width, classes * width), BF),
            pltpu.VMEM((2, width + 8, 2 * LANES), F32),
            pltpu.VMEM((2, width + 8, 2 * LANES), F32),
            pltpu.VMEM((2, width + 8, 2 * LANES), F32),
            pltpu.VMEM((2, 2, width + 8, LANES), F32),
            pltpu.VMEM((2, width + 8, 2 * LANES), F32),
            pltpu.VMEM((2, wide, LANES), F32),
            pltpu.VMEM((classes, 2, width // 2 + 16, 2 * LANES), BF),
            pltpu.VMEM((2, 2 * LANES, 2 * LANES), BF),
            pltpu.VMEM((2, 2, width + 16, 2 * LANES), BF),
            pltpu.VMEM((2, 2, readout + 16, 2 * LANES), BF),
            pltpu.VMEM((2, 2 * readout, 2 * LANES), BF),
            pltpu.SemaphoreType.DMA((len(operands) + coils.shape[0],)),
        ],
        compiler_params=pltpu.CompilerParams(vmem_limit_bytes=40 * 2**20),
        name="normal_operator",
    )(*[pltpu.with_memory_space_constraint(a, pltpu.HBM) for a in operands])


def from_partner(value, axis, apart):
    mask = 2**apart
    pairs = [(source, source ^ mask) for source in range(lax.axis_size(axis))]
    return lax.ppermute(value, axis, pairs)


def gather_slice(values, bit_count, device_rank):
    for bit_index in range(bit_count):
        partner = from_partner(values, "space", bit_index)
        low_side = device_rank >> bit_index & 1 == 0
        values = jnp.where(
            low_side, jnp.concatenate([values, partner], 0), jnp.concatenate([partner, values], 0)
        )
    return values


def sum_slice(values, bit_count, device_rank):
    for bit_index in reversed(range(bit_count)):
        half_rows = values.shape[0] // 2
        low_side = device_rank >> bit_index & 1 == 0
        kept_part = jnp.where(low_side, values[:half_rows], values[half_rows:])
        sent_part = jnp.where(low_side, values[half_rows:], values[:half_rows])
        values = kept_part + from_partner(sent_part, "space", bit_index)
    return values


def regroup_coils(coil_maps, bit_count, device_rank):
    group_size = 1 << bit_count
    pieces = coil_maps.reshape((group_size, coil_maps.shape[0] // group_size) + coil_maps.shape[1:])
    for bit_index in range(bit_count):
        old_shape = pieces.shape
        halves = pieces.reshape((group_size >> bit_index + 1, 2, 1 << bit_index) + old_shape[1:])
        low_side = device_rank >> bit_index & 1 == 0
        kept_part = jnp.where(low_side, halves[:, 0], halves[:, 1])
        sent_part = jnp.where(low_side, halves[:, 1], halves[:, 0])
        partner = from_partner(sent_part, "space", bit_index)
        pieces = jnp.stack(
            [jnp.where(low_side, kept_part, partner), jnp.where(low_side, partner, kept_part)], 1
        ).reshape(old_shape)
    moved = jnp.moveaxis(pieces, 0, 1)
    return moved.reshape((moved.shape[0], group_size * coil_maps.shape[1]) + coil_maps.shape[2:])


def on_device(image, coil_maps, psf_phase, line_mask, motion):
    lines = image.shape[0]
    length = line_mask.shape[1]
    device_rank = lax.axis_index("space")
    group_size = max(1, length // lines)
    bit_count = group_size.bit_length() - 1
    if bit_count:
        coil_maps = regroup_coils(coil_maps, bit_count, device_rank)
        psf_phase = gather_slice(psf_phase, bit_count, device_rank)
        image = gather_slice(image, bit_count, device_rank)
    image = jnp.transpose(image, (1, 2, 0))
    coil_maps = jnp.transpose(coil_maps, (0, 2, 3, 1))
    results = []
    for start in range(0, image.shape[2], length):
        stop = start + length
        results.append(
            slice_operator(
                motion, line_mask, image[:, :, start:stop], psf_phase[start:stop], coil_maps[..., start:stop]
            )
        )
    result = results[0] if len(results) == 1 else jnp.concatenate(results, 2)
    if bit_count:
        result = jnp.transpose(result, (2, 0, 1))
        result = sum_slice(result, bit_count, device_rank)
        result = jnp.transpose(result, (1, 2, 0))
    shots = lax.axis_size("shot")
    total = result
    for apart in range(1, shots):
        pairs = [(source, (source + apart) % shots) for source in range(shots)]
        total = total + lax.ppermute(result, "shot", pairs)
    return jnp.transpose(total, (2, 0, 1))


def solution(mesh):
    in_specs = (
        P(("parts", "space"), None, None),
        P(None, ("parts", "space"), None, None),
        P(("parts", "space"), None),
        P(("parts", "shot"), None),
        P(("parts", "shot"), None),
    )
    out_specs = P(("parts", "space"), None, None)
    return jax.shard_map(
        on_device, mesh=mesh, in_specs=in_specs, out_specs=out_specs, check_vma=False
    )
```

```python
import functools

import jax
import jax.numpy as jnp
import numpy as np
from jax import lax
from jax.experimental import pallas as pl
from jax.experimental.pallas import tpu as pltpu
from jax.sharding import PartitionSpec as P

LEVELS = 17
ANGLE_STEP = 0.02
SHIFT_STEP = 0.5
LANES = 128
UNROLL = 7
BF = jnp.bfloat16
F32 = jnp.float32


def split_pair(table):
    high = table.astype(np.float32).astype(BF)
    low = (table - high.astype(np.float64)).astype(np.float32).astype(BF)
    return np.stack([high, low])


def row_tables(width):
    half = width // 2
    result = []
    for parity in range(2):
        freqs = 2 * np.arange(half)[:, None] + parity
        wave = np.exp(-2j * np.pi * (freqs * np.arange(half)[None, :] % width) / width) / np.sqrt(width)
        table = np.block([[wave.real, -wave.imag], [wave.imag, wave.real]])
        result.append(split_pair(table))
    return np.stack(result)


def column_tables(length):
    half = length // 2
    result = []
    for parity in range(2):
        inputs = np.arange(half)[:, None]
        freqs = 2 * np.arange(half)[None, :] + parity
        angle = -2 * np.pi * (inputs * freqs % length) / length
        wave = np.exp(1j * angle) / np.sqrt(length)
        table = np.zeros((2 * LANES, 2 * LANES))
        table[:half, :half] = wave.real
        table[:half, LANES:LANES + half] = wave.imag
        table[LANES:LANES + half, :half] = -wave.imag
        table[LANES:LANES + half, LANES:LANES + half] = wave.real
        result.append(split_pair(table))
    return np.stack(result)


def readout_tables(width, readout):
    half = width // 2
    classes = readout // half
    pads = []
    for j in range(classes):
        k = np.arange(half)[:, None] * classes + j
        x = np.arange(half)[None, :]
        angle = -2 * np.pi * (k * x % readout) / readout
        cosine = (np.cos(angle) / np.sqrt(readout)).astype(np.float32).astype(BF)
        sine = (np.sin(angle) / np.sqrt(readout)).astype(np.float32).astype(BF)
        pads.append(np.block([[cosine, -sine], [sine, cosine]]))
    return np.stack(pads)


def turn_polys(degree):
    nodes = np.cos(np.pi * (np.arange(400) + 0.5) / 400) * 0.125 + 0.125
    root = np.sqrt(nodes)
    out = []
    for value in (np.cos(2 * np.pi * root), np.sin(2 * np.pi * root) / root):
        series = np.polynomial.chebyshev.Chebyshev.fit(nodes, value, degree, domain=[0, 0.25])
        out.append([float(c) for c in series.convert(kind=np.polynomial.Polynomial).coef])
    return out


FULL_POLY, WAVE_POLY = turn_polys(6), turn_polys(5)


def turn_pair(turns, poly=FULL_POLY):
    cos_poly, sin_poly = poly
    square = turns * turns
    cosine = jnp.full_like(square, cos_poly[-1])
    sine = jnp.full_like(square, sin_poly[-1])
    for c, s in zip(cos_poly[-2::-1], sin_poly[-2::-1]):
        cosine = cosine * square + c
        sine = sine * square + s
    return cosine, sine * turns


def wrap(turns):
    return turns - jnp.floor(turns + 0.5)


def dot(left, right):
    return jnp.dot(left, right, preferred_element_type=F32)


def dot_nt(left, right):
    return lax.dot_general(left, right, (((1,), (1,)), ((), ())), preferred_element_type=F32)


def two(value):
    high = value.astype(BF)
    return high, (value - high.astype(F32)).astype(BF)


def spread(value, length):
    half = length // 2
    blank = jnp.zeros((value.shape[0], LANES - half), value.dtype)
    return jnp.concatenate([value[:, :half], blank, value[:, half:], blank], 1)


def table_rows(table_ref, value):
    high, low = two(value)
    th, tl = table_ref[0], table_ref[1]
    return dot(th, high) + dot(tl, high) + dot(th, low)


def shear_rows(re, im, tx_ref, txt_ref, phase_ref, sign):
    half = re.shape[0] // 2
    back = []
    for parity in range(2):
        join = (lambda v: v[:half] - v[half:]) if parity else (lambda v: v[:half] + v[half:])
        spectra = table_rows(tx_ref.at[parity], jnp.concatenate([join(re), join(im)], 0))
        sr, si = spectra[:half], spectra[half:]
        rows = slice(parity * half, (parity + 1) * half)
        c, s = phase_ref[0, rows], phase_ref[1, rows] * sign
        back.append(table_rows(txt_ref.at[parity], jnp.concatenate([sr * c - si * s, sr * s + si * c], 0)))
    even, odd = back
    low, high = even + odd, even - odd
    return jnp.concatenate([low[:half], high[:half]], 0), jnp.concatenate([low[half:], high[half:]], 0)


def shear_columns(re, im, ty_ref, phase_ref, sign):
    width = re.shape[0]
    back = []
    for parity in range(2):
        join = (lambda v: v[:, :LANES] - v[:, LANES:]) if parity else (lambda v: v[:, :LANES] + v[:, LANES:])
        high, low = two(jnp.concatenate([join(re), join(im)], 1))
        th, tl = ty_ref[parity, 0], ty_ref[parity, 1]
        spectra = dot(high, th) + dot(low, th) + dot(high, tl)
        sr, si = spectra[:, :LANES], spectra[:, LANES:]
        c, s = phase_ref[parity, 0, :width], phase_ref[parity, 1, :width] * sign
        high, low = two(jnp.concatenate([sr * c - si * s, sr * s + si * c], 1))
        back.append(dot_nt(high, th) + dot_nt(low, th) + dot_nt(high, tl))
    even, odd = back
    low_half, high_half = even + odd, even - odd
    return (
        jnp.concatenate([low_half[:, :LANES], high_half[:, :LANES]], 1),
        jnp.concatenate([low_half[:, LANES:], high_half[:, LANES:]], 1),
    )


def signed(counter, length):
    return jnp.where(counter < length // 2, counter, counter - length).astype(F32)


def put(ref, re, im):
    ref[0, :re.shape[0]] = re
    ref[1, :im.shape[0]] = im


def make_phases(motion_ref, p1_ref, pc_ref, p3_ref, width, length):
    half = length // 2
    center = (LEVELS - 1) / 2.0
    shift_x = (motion_ref[0, 1].astype(F32) - center) * SHIFT_STEP
    shift_y = (motion_ref[0, 2].astype(F32) - center) * SHIFT_STEP
    angle = jnp.full((8, LANES), (motion_ref[0, 0].astype(F32) - center) * ANGLE_STEP, F32)
    tilt = jnp.sin(angle)[:1, :1]
    slope = -(jnp.sin(angle * 0.5) / jnp.cos(angle * 0.5))[:1, :1]
    lane = lax.broadcasted_iota(jnp.int32, (1, 2 * LANES), 1)
    line = jnp.where(lane < LANES, lane, lane - LANES + half)
    bend = slope * (line.astype(F32) - length / 2.0)
    side = width // 2
    coarse = signed(16 * lax.broadcasted_iota(jnp.int32, (-(-side // 64) * 8, 1), 0), width) * (-1.0 / width)
    fine = (2 * lax.broadcasted_iota(jnp.int32, (8, 1), 0)).astype(F32)
    for ref, shift in ((p1_ref, bend + shift_x), (p3_ref, bend)):
        gc, gs = turn_pair(wrap(coarse * shift))
        for parity in range(2):
            c, s = turn_pair(wrap((fine + parity) * (-1.0 / width) * shift))
            for a in range(side // 8):
                rows = pl.ds(parity * side + 8 * a, 8)
                ac, as_ = gc[a:a + 1], gs[a:a + 1]
                ref[0, rows] = c * ac - s * as_
                ref[1, rows] = c * as_ + s * ac
    lane = lax.broadcasted_iota(jnp.int32, (1, LANES), 1)
    coarse = (8 * lax.broadcasted_iota(jnp.int32, (-(-width // 64) * 8, 1), 0)).astype(F32) - width / 2.0
    fine = lax.broadcasted_iota(jnp.int32, (8, 1), 0).astype(F32)
    for parity in range(2):
        freq = signed(2 * lane + parity, length) * (-1.0 / length)
        gc, gs = turn_pair(wrap((tilt * coarse + shift_y) * freq))
        c, s = turn_pair(wrap(tilt * fine * freq))
        for a in range(width // 8):
            rows = pl.ds(8 * a, 8)
            ac, as_ = gc[a:a + 1], gs[a:a + 1]
            pc_ref[parity, 0, rows] = c * ac - s * as_
            pc_ref[parity, 1, rows] = c * as_ + s * ac


def make_projector(mask_ref, ty_ref, h_ref, length):
    half = length // 2
    mask = jnp.broadcast_to(mask_ref[...].astype(F32), (8, length)).astype(BF)
    line = lax.broadcasted_iota(jnp.int32, (length, 2 * LANES), 0)
    lane = lax.broadcasted_iota(jnp.int32, (length, 2 * LANES), 1) % LANES
    picked = []
    for parity in range(2):
        select = jnp.where((line == 2 * lane + parity) & (lane < half), 1.0, 0.0).astype(BF)
        picked.append(dot(mask, select)[:1])
    counts = [jnp.sum(p[:, :LANES], 1, keepdims=True) for p in picked]
    total = ((counts[0] + counts[1]) / length).astype(BF).astype(F32)
    larger = (jnp.maximum(counts[0], counts[1]) / length).astype(BF).astype(F32)
    rest = total - larger
    row = lax.broadcasted_iota(jnp.int32, (2 * LANES, 2 * LANES), 0)
    col = lax.broadcasted_iota(jnp.int32, (2 * LANES, 2 * LANES), 1)
    diagonal = (row == col) & (row % LANES < half)
    for parity in range(2):
        th, tl = ty_ref[parity, 0], ty_ref[parity, 1]
        keep = picked[parity]
        mh = (th.astype(F32) * keep).astype(BF)
        ml = (tl.astype(F32) * keep).astype(BF)
        table = dot_nt(mh, th) + dot_nt(ml, th) + dot_nt(mh, tl)
        value = jnp.where(counts[parity] >= counts[1 - parity], larger, rest)
        if parity:
            value = jnp.where(counts[1] > counts[0], larger, rest)
        h_ref[parity] = jnp.where(diagonal, value, table).astype(BF)


def make_wave(psf_ref, psft_ref, wave_ref, length, classes):
    half = length // 2
    readout = psf_ref.shape[1]
    blank = jnp.zeros((LANES - half, readout), F32)
    psf = jnp.concatenate([psf_ref[:half], blank, psf_ref[half:], blank], 0) * (0.5 / np.pi)
    wide = -(-readout // LANES) * LANES
    if wide > readout:
        psf = jnp.concatenate([psf, jnp.zeros((2 * LANES, wide - readout), F32)], 1)
    for side in range(2):
        psft_ref[side] = psf[side * LANES:(side + 1) * LANES].T
    rows = readout // classes
    for j in range(classes):
        picked = pl.ds(j, rows, stride=classes)
        c, s = turn_pair(jnp.concatenate([psft_ref[0, picked, :], psft_ref[1, picked, :]], 1), WAVE_POLY)
        put(wave_ref.at[j], c.astype(BF), s.astype(BF))


def make_inverse_rows(tx_ref, txt_ref):
    for parity in range(2):
        for part in range(2):
            txt_ref[parity, part] = tx_ref[parity, part].astype(F32).T.astype(BF)


def make_crop(pt_ref, ct_ref, half, classes):
    for j in range(classes):
        back = pt_ref[j].astype(F32).T
        re, im = back[:half], back[half:]
        angle = 2 * np.pi * j / classes
        wr, wi = float(np.cos(angle)), float(np.sin(angle))
        columns = pl.ds(2 * half * j, 2 * half)
        ct_ref[pl.ds(0, half), columns] = re.astype(BF)
        ct_ref[pl.ds(half, half), columns] = (re * wr - im * wi).astype(BF)
        ct_ref[pl.ds(2 * half, half), columns] = im.astype(BF)
        ct_ref[pl.ds(3 * half, half), columns] = (re * wi + im * wr).astype(BF)


def encode(coil, rot_ref, pt_ref, wave_ref, c_ref, w_ref, length, classes):
    width = coil.shape[1]
    half = width // 2
    cr = spread(coil[0], length)
    ci = spread(coil[1], length)
    put(c_ref, cr, ci)
    rr, ri = rot_ref[0, :width], rot_ref[1, :width]
    zr = (cr.astype(F32) * rr - ci.astype(F32) * ri).astype(BF)
    zi = (cr.astype(F32) * ri + ci.astype(F32) * rr).astype(BF)
    ar, ai, br, bi = zr[:half], zi[:half], zr[half:], zi[half:]
    for j in range(classes // 2):
        angle = -2 * np.pi * j / classes
        wr, wi = float(np.cos(angle)), float(np.sin(angle))
        if j == 0:
            ur, ui = br, bi
        else:
            ur, ui = br * wr - bi * wi, br * wi + bi * wr
        for step in range(2):
            cls = j + step * (classes // 2)
            tr, ti = (ar - ur, ai - ui) if step else (ar + ur, ai + ui)
            spectra = dot(pt_ref[cls], jnp.concatenate([tr, ti], 0)).astype(BF)
            sr, si = spectra[:half], spectra[half:]
            c, s = wave_ref[cls, 0, :half], wave_ref[cls, 1, :half]
            vr = sr * c - si * s
            vi = sr * s + si * c
            rows = pl.ds(cls * half, half)
            w_ref[0, rows, :LANES] = vr[:, :LANES] + vr[:, LANES:]
            w_ref[0, rows, LANES:] = vi[:, :LANES] + vi[:, LANES:]
            w_ref[1, rows, :LANES] = vr[:, :LANES] - vr[:, LANES:]
            w_ref[1, rows, LANES:] = vi[:, :LANES] - vi[:, LANES:]


def project(wave_ref, h_ref, w_ref, u_ref, half, classes):
    readout = classes * half
    third = readout // 3
    pieces = [
        (dot(w_ref[0, i:i + third], h_ref[0]).astype(BF), dot(w_ref[1, i:i + third], h_ref[1]).astype(BF))
        for i in range(0, readout, third)
    ]
    for cls in range(classes):
        plus, minus = pieces[cls * half // third]
        rows = slice(cls * half % third, cls * half % third + half)
        for side, y in enumerate((plus[rows] + minus[rows], plus[rows] - minus[rows])):
            lanes = slice(side * LANES, (side + 1) * LANES)
            yr, yi = y[:, :LANES], y[:, LANES:]
            c, s = wave_ref[cls, 0, :half, lanes], wave_ref[cls, 1, :half, lanes]
            u_ref[pl.ds(2 * cls * half, half), lanes] = yr * c + yi * s
            u_ref[pl.ds((2 * cls + 1) * half, half), lanes] = yi * c - yr * s


def decode(acc_ref, ct_ref, c_ref, u_ref, width):
    back = dot(ct_ref[...], u_ref[...])
    br, bi = back[:width].astype(BF), back[width:].astype(BF)
    cr, ci = c_ref[0, :width], c_ref[1, :width]
    acc_ref[0, :width] += (cr * br + ci * bi).astype(F32)
    acc_ref[1, :width] += (cr * bi - ci * br).astype(F32)


def kernel(
    motion_hbm, mask_hbm, image_hbm, tx_hbm, ty_hbm, psf_hbm, pt_hbm, coil_hbm, out_ref,
    motion_ref, mask_ref, image_ref, tx_ref, ty_ref, psf_ref, pt_ref, coil_ref,
    txt_ref, ct_ref, rot_ref, acc_ref, p1_ref, pc_ref, p3_ref, psft_ref, wave_ref, h_ref, c_ref, w_ref, u_ref, sems,
    *, length, classes, unroll,
):
    width = image_ref.shape[1]
    half = length // 2
    sources = (motion_hbm, mask_hbm, image_hbm, tx_hbm, ty_hbm, psf_hbm, pt_hbm)
    targets = (motion_ref, mask_ref, image_ref, tx_ref, ty_ref, psf_ref, pt_ref)
    copies = [pltpu.make_async_copy(a, b, sems.at[i]) for i, (a, b) in enumerate(zip(sources, targets))]
    count = coil_ref.shape[0]
    chunk = 2 - count % 2

    def coil_copy(index):
        part = pl.ds(index * chunk, chunk)
        return pltpu.make_async_copy(coil_hbm.at[part], coil_ref.at[part], sems.at[len(sources) + index])

    for copy in copies:
        copy.start()
    copies[0].wait()
    make_phases(motion_ref, p1_ref, pc_ref, p3_ref, width, length)
    for copy in copies[1:4]:
        copy.wait()
    for index in range(count // chunk):
        coil_copy(index).start()
    make_inverse_rows(tx_ref, txt_ref)
    re, im = spread(image_ref[0], length), spread(image_ref[1], length)
    re, im = shear_rows(re, im, tx_ref, txt_ref, p1_ref, 1.0)
    acc_ref[...] = jnp.zeros_like(acc_ref)
    for copy in copies[4:]:
        copy.wait()
    make_crop(pt_ref, ct_ref, width // 2, classes)
    make_projector(mask_ref, ty_ref, h_ref, length)
    re, im = shear_columns(re, im, ty_ref, pc_ref, 1.0)
    re, im = shear_rows(re, im, tx_ref, txt_ref, p3_ref, 1.0)
    make_wave(psf_ref, psft_ref, wave_ref, length, classes)
    put(rot_ref, re, im)
    for index in range(count // chunk):
        coil_copy(index).wait()

    def run(stage, coil):
        slot = coil % 2 if isinstance(coil, int) else coil[1]
        index = coil if isinstance(coil, int) else coil[0]
        if stage == 0:
            encode(coil_ref[index], rot_ref, pt_ref, wave_ref, c_ref.at[slot], w_ref.at[slot], length, classes)
        elif stage == 1:
            project(wave_ref, h_ref, w_ref.at[slot], u_ref.at[slot], width // 2, classes)
        else:
            decode(acc_ref, ct_ref, c_ref.at[slot], u_ref.at[slot], width)

    def pair(first):
        run(2, (first - 2, 0))
        run(1, (first - 1, 1))
        run(0, (first, 0))
        run(2, (first - 1, 1))
        run(1, (first, 0))
        run(0, (first + 1, 1))

    if count % 2:
        def single(coil, carry):
            for stage in range(3):
                run(stage, (coil, 0))
            return carry

        lax.fori_loop(0, count, single, 0)
    else:
        pairs = count // 2 - 1
        run(0, 0)
        run(1, 0)
        run(0, 1)
        steps = pairs // unroll
        for extra in range(pairs - steps * unroll):
            pair(2 * extra + 2)

        def some_pairs(step, carry):
            for inner in range(unroll):
                pair(2 * (pairs - steps * unroll + step * unroll + inner) + 2)
            return carry

        if steps:
            lax.fori_loop(0, steps, some_pairs, 0)
        run(2, count - 2)
        run(1, count - 1)
        run(2, count - 1)

    re, im = acc_ref[0, :width], acc_ref[1, :width]
    re, im = shear_rows(re, im, tx_ref, txt_ref, p3_ref, -1.0)
    re, im = shear_columns(re, im, ty_ref, pc_ref, -1.0)
    re, im = shear_rows(re, im, tx_ref, txt_ref, p1_ref, -1.0)
    for part, value in enumerate((re, im)):
        out_ref[part] = jnp.concatenate([value[:, :half], value[:, LANES:LANES + half]], 1)


def slice_operator(motion, mask, image, psf, coils):
    _, width, length = image.shape
    readout = psf.shape[1]
    classes = readout // (width // 2)
    pads = readout_tables(width, readout)
    tx, ty = row_tables(width), column_tables(length)
    wide = -(-readout // LANES) * LANES
    operands = (motion, mask, image, jnp.asarray(tx), jnp.asarray(ty), psf, jnp.asarray(pads), coils)
    return pl.pallas_call(
        functools.partial(kernel, length=length, classes=classes, unroll=UNROLL),
        in_specs=[pl.BlockSpec(memory_space=pltpu.HBM) for _ in operands],
        out_specs=pl.BlockSpec(memory_space=pltpu.VMEM),
        out_shape=jax.ShapeDtypeStruct(image.shape, F32),
        scratch_shapes=[pltpu.SMEM(motion.shape, motion.dtype)]
        + [pltpu.VMEM(a.shape, a.dtype) for a in operands[1:]]
        + [
            pltpu.VMEM(tx.shape, BF),
            pltpu.VMEM((2 * width, classes * width), BF),
            pltpu.VMEM((2, width + 8, 2 * LANES), F32),
            pltpu.VMEM((2, width + 8, 2 * LANES), F32),
            pltpu.VMEM((2, width + 8, 2 * LANES), F32),
            pltpu.VMEM((2, 2, width + 8, LANES), F32),
            pltpu.VMEM((2, width + 8, 2 * LANES), F32),
            pltpu.VMEM((2, wide, LANES), F32),
            pltpu.VMEM((classes, 2, width // 2 + 16, 2 * LANES), BF),
            pltpu.VMEM((2, 2 * LANES, 2 * LANES), BF),
            pltpu.VMEM((2, 2, width + 16, 2 * LANES), BF),
            pltpu.VMEM((2, 2, readout + 16, 2 * LANES), BF),
            pltpu.VMEM((2, 2 * readout, 2 * LANES), BF),
            pltpu.SemaphoreType.DMA((len(operands) + coils.shape[0],)),
        ],
        compiler_params=pltpu.CompilerParams(vmem_limit_bytes=40 * 2**20),
        name="normal_operator",
    )(*[pltpu.with_memory_space_constraint(a, pltpu.HBM) for a in operands])


def from_partner(value, axis, apart):
    mask = 2**apart
    pairs = [(source, source ^ mask) for source in range(lax.axis_size(axis))]
    return lax.ppermute(value, axis, pairs)


def gather_slice(values, bit_count, device_rank):
    for bit_index in range(bit_count):
        partner = from_partner(values, "space", bit_index)
        low_side = device_rank >> bit_index & 1 == 0
        values = jnp.where(
            low_side, jnp.concatenate([values, partner], 0), jnp.concatenate([partner, values], 0)
        )
    return values


def sum_slice(values, bit_count, device_rank):
    for bit_index in reversed(range(bit_count)):
        half_rows = values.shape[0] // 2
        low_side = device_rank >> bit_index & 1 == 0
        kept_part = jnp.where(low_side, values[:half_rows], values[half_rows:])
        sent_part = jnp.where(low_side, values[half_rows:], values[:half_rows])
        values = kept_part + from_partner(sent_part, "space", bit_index)
    return values


def regroup_coils(coil_maps, bit_count, device_rank):
    group_size = 1 << bit_count
    pieces = coil_maps.reshape((group_size, coil_maps.shape[0] // group_size) + coil_maps.shape[1:])
    for bit_index in range(bit_count):
        old_shape = pieces.shape
        halves = pieces.reshape((group_size >> bit_index + 1, 2, 1 << bit_index) + old_shape[1:])
        low_side = device_rank >> bit_index & 1 == 0
        kept_part = jnp.where(low_side, halves[:, 0], halves[:, 1])
        sent_part = jnp.where(low_side, halves[:, 1], halves[:, 0])
        partner = from_partner(sent_part, "space", bit_index)
        pieces = jnp.stack(
            [jnp.where(low_side, kept_part, partner), jnp.where(low_side, partner, kept_part)], 1
        ).reshape(old_shape)
    moved = jnp.moveaxis(pieces, 0, 1)
    return moved.reshape((moved.shape[0], group_size * coil_maps.shape[1]) + coil_maps.shape[2:])


def on_device(image, coil_maps, psf_phase, line_mask, motion):
    lines = image.shape[0]
    length = line_mask.shape[1]
    device_rank = lax.axis_index("space")
    group_size = max(1, length // lines)
    bit_count = group_size.bit_length() - 1
    if bit_count:
        coil_maps = regroup_coils(coil_maps, bit_count, device_rank)
        psf_phase = gather_slice(psf_phase, bit_count, device_rank)
        image = gather_slice(image, bit_count, device_rank)
    image = jnp.transpose(image, (1, 2, 0))
    coil_maps = jnp.transpose(coil_maps, (0, 2, 3, 1))
    results = []
    for start in range(0, image.shape[2], length):
        stop = start + length
        results.append(
            slice_operator(
                motion, line_mask, image[:, :, start:stop], psf_phase[start:stop], coil_maps[..., start:stop]
            )
        )
    result = results[0] if len(results) == 1 else jnp.concatenate(results, 2)
    if bit_count:
        result = jnp.transpose(result, (2, 0, 1))
        result = sum_slice(result, bit_count, device_rank)
        result = jnp.transpose(result, (1, 2, 0))
    shots = lax.axis_size("shot")
    total = result
    for apart in range(1, shots):
        pairs = [(source, (source + apart) % shots) for source in range(shots)]
        total = total + lax.ppermute(result, "shot", pairs)
    return jnp.transpose(total, (2, 0, 1))


def solution(mesh):
    in_specs = (
        P(("parts", "space"), None, None),
        P(None, ("parts", "space"), None, None),
        P(("parts", "space"), None),
        P(("parts", "shot"), None),
        P(("parts", "shot"), None),
    )
    out_specs = P(("parts", "space"), None, None)
    return jax.shard_map(
        on_device, mesh=mesh, in_specs=in_specs, out_specs=out_specs, check_vma=False
    )
```

```python
import functools

import jax
import jax.numpy as jnp
import numpy as np
from jax import lax
from jax.experimental import pallas as pl
from jax.experimental.pallas import tpu as pltpu
from jax.sharding import PartitionSpec as P

LEVELS = 17
ANGLE_STEP = 0.02
SHIFT_STEP = 0.5
LANES = 128
UNROLL = 7
BF = jnp.bfloat16
F32 = jnp.float32


def split_pair(table):
    high = table.astype(np.float32).astype(BF)
    low = (table - high.astype(np.float64)).astype(np.float32).astype(BF)
    return np.stack([high, low])


def row_tables(width):
    half = width // 2
    result = []
    for parity in range(2):
        freqs = 2 * np.arange(half)[:, None] + parity
        wave = np.exp(-2j * np.pi * (freqs * np.arange(half)[None, :] % width) / width) / np.sqrt(width)
        table = np.block([[wave.real, -wave.imag], [wave.imag, wave.real]])
        result.append(split_pair(table))
    return np.stack(result)


def column_tables(length):
    half = length // 2
    result = []
    for parity in range(2):
        inputs = np.arange(half)[:, None]
        freqs = 2 * np.arange(half)[None, :] + parity
        angle = -2 * np.pi * (inputs * freqs % length) / length
        wave = np.exp(1j * angle) / np.sqrt(length)
        table = np.zeros((2 * LANES, 2 * LANES))
        table[:half, :half] = wave.real
        table[:half, LANES:LANES + half] = wave.imag
        table[LANES:LANES + half, :half] = -wave.imag
        table[LANES:LANES + half, LANES:LANES + half] = wave.real
        result.append(split_pair(table))
    return np.stack(result)


def readout_tables(width, readout):
    half = width // 2
    classes = readout // half
    pads = []
    for j in range(classes):
        k = np.arange(half)[:, None] * classes + j
        x = np.arange(half)[None, :]
        angle = -2 * np.pi * (k * x % readout) / readout
        cosine = (np.cos(angle) / np.sqrt(readout)).astype(np.float32).astype(BF)
        sine = (np.sin(angle) / np.sqrt(readout)).astype(np.float32).astype(BF)
        pads.append(np.block([[cosine, -sine], [sine, cosine]]))
    return np.stack(pads)


def turn_polys(degree):
    nodes = np.cos(np.pi * (np.arange(400) + 0.5) / 400) * 0.125 + 0.125
    root = np.sqrt(nodes)
    out = []
    for value in (np.cos(2 * np.pi * root), np.sin(2 * np.pi * root) / root):
        series = np.polynomial.chebyshev.Chebyshev.fit(nodes, value, degree, domain=[0, 0.25])
        out.append([float(c) for c in series.convert(kind=np.polynomial.Polynomial).coef])
    return out


FULL_POLY, WAVE_POLY = turn_polys(6), turn_polys(5)


def turn_pair(turns, poly=FULL_POLY):
    cos_poly, sin_poly = poly
    square = turns * turns
    cosine = jnp.full_like(square, cos_poly[-1])
    sine = jnp.full_like(square, sin_poly[-1])
    for c, s in zip(cos_poly[-2::-1], sin_poly[-2::-1]):
        cosine = cosine * square + c
        sine = sine * square + s
    return cosine, sine * turns


def wrap(turns):
    return turns - jnp.floor(turns + 0.5)


def dot(left, right):
    return jnp.dot(left, right, preferred_element_type=F32)


def dot_nt(left, right):
    return lax.dot_general(left, right, (((1,), (1,)), ((), ())), preferred_element_type=F32)


def two(value):
    high = value.astype(BF)
    return high, (value - high.astype(F32)).astype(BF)


def spread(value, length):
    half = length // 2
    blank = jnp.zeros((value.shape[0], LANES - half), value.dtype)
    return jnp.concatenate([value[:, :half], blank, value[:, half:], blank], 1)


def table_rows(table_ref, value):
    high, low = two(value)
    th, tl = table_ref[0], table_ref[1]
    return dot(th, high) + dot(tl, high) + dot(th, low)


def shear_rows(re, im, tx_ref, txt_ref, phase_ref, sign):
    half = re.shape[0] // 2
    back = []
    for parity in range(2):
        join = (lambda v: v[:half] - v[half:]) if parity else (lambda v: v[:half] + v[half:])
        spectra = table_rows(tx_ref.at[parity], jnp.concatenate([join(re), join(im)], 0))
        sr, si = spectra[:half], spectra[half:]
        rows = slice(parity * half, (parity + 1) * half)
        c, s = phase_ref[0, rows], phase_ref[1, rows] * sign
        back.append(table_rows(txt_ref.at[parity], jnp.concatenate([sr * c - si * s, sr * s + si * c], 0)))
    even, odd = back
    low, high = even + odd, even - odd
    return jnp.concatenate([low[:half], high[:half]], 0), jnp.concatenate([low[half:], high[half:]], 0)


def shear_columns(re, im, ty_ref, phase_ref, sign):
    width = re.shape[0]
    back = []
    for parity in range(2):
        join = (lambda v: v[:, :LANES] - v[:, LANES:]) if parity else (lambda v: v[:, :LANES] + v[:, LANES:])
        high, low = two(jnp.concatenate([join(re), join(im)], 1))
        th, tl = ty_ref[parity, 0], ty_ref[parity, 1]
        spectra = dot(high, th) + dot(low, th) + dot(high, tl)
        sr, si = spectra[:, :LANES], spectra[:, LANES:]
        c, s = phase_ref[parity, 0, :width], phase_ref[parity, 1, :width] * sign
        high, low = two(jnp.concatenate([sr * c - si * s, sr * s + si * c], 1))
        back.append(dot_nt(high, th) + dot_nt(low, th) + dot_nt(high, tl))
    even, odd = back
    low_half, high_half = even + odd, even - odd
    return (
        jnp.concatenate([low_half[:, :LANES], high_half[:, :LANES]], 1),
        jnp.concatenate([low_half[:, LANES:], high_half[:, LANES:]], 1),
    )


def signed(counter, length):
    return jnp.where(counter < length // 2, counter, counter - length).astype(F32)


def put(ref, re, im):
    ref[0, :re.shape[0]] = re
    ref[1, :im.shape[0]] = im


def make_phases(motion_ref, p1_ref, pc_ref, p3_ref, width, length):
    half = length // 2
    center = (LEVELS - 1) / 2.0
    shift_x = (motion_ref[0, 1].astype(F32) - center) * SHIFT_STEP
    shift_y = (motion_ref[0, 2].astype(F32) - center) * SHIFT_STEP
    angle = jnp.full((8, LANES), (motion_ref[0, 0].astype(F32) - center) * ANGLE_STEP, F32)
    tilt = jnp.sin(angle)[:1, :1]
    slope = -(jnp.sin(angle * 0.5) / jnp.cos(angle * 0.5))[:1, :1]
    lane = lax.broadcasted_iota(jnp.int32, (1, 2 * LANES), 1)
    line = jnp.where(lane < LANES, lane, lane - LANES + half)
    bend = slope * (line.astype(F32) - length / 2.0)
    side = width // 2
    coarse = signed(16 * lax.broadcasted_iota(jnp.int32, (-(-side // 64) * 8, 1), 0), width) * (-1.0 / width)
    fine = (2 * lax.broadcasted_iota(jnp.int32, (8, 1), 0)).astype(F32)
    for ref, shift in ((p1_ref, bend + shift_x), (p3_ref, bend)):
        gc, gs = turn_pair(wrap(coarse * shift))
        for parity in range(2):
            c, s = turn_pair(wrap((fine + parity) * (-1.0 / width) * shift))
            for a in range(side // 8):
                rows = pl.ds(parity * side + 8 * a, 8)
                ac, as_ = gc[a:a + 1], gs[a:a + 1]
                ref[0, rows] = c * ac - s * as_
                ref[1, rows] = c * as_ + s * ac
    lane = lax.broadcasted_iota(jnp.int32, (1, LANES), 1)
    coarse = (8 * lax.broadcasted_iota(jnp.int32, (-(-width // 64) * 8, 1), 0)).astype(F32) - width / 2.0
    fine = lax.broadcasted_iota(jnp.int32, (8, 1), 0).astype(F32)
    for parity in range(2):
        freq = signed(2 * lane + parity, length) * (-1.0 / length)
        gc, gs = turn_pair(wrap((tilt * coarse + shift_y) * freq))
        c, s = turn_pair(wrap(tilt * fine * freq))
        for a in range(width // 8):
            rows = pl.ds(8 * a, 8)
            ac, as_ = gc[a:a + 1], gs[a:a + 1]
            pc_ref[parity, 0, rows] = c * ac - s * as_
            pc_ref[parity, 1, rows] = c * as_ + s * ac


def make_projector(mask_ref, ty_ref, h_ref, length):
    half = length // 2
    mask = jnp.broadcast_to(mask_ref[...].astype(F32), (8, length)).astype(BF)
    line = lax.broadcasted_iota(jnp.int32, (length, 2 * LANES), 0)
    lane = lax.broadcasted_iota(jnp.int32, (length, 2 * LANES), 1) % LANES
    picked = []
    for parity in range(2):
        select = jnp.where((line == 2 * lane + parity) & (lane < half), 1.0, 0.0).astype(BF)
        picked.append(dot(mask, select)[:1])
    counts = [jnp.sum(p[:, :LANES], 1, keepdims=True) for p in picked]
    total = ((counts[0] + counts[1]) / length).astype(BF).astype(F32)
    larger = (jnp.maximum(counts[0], counts[1]) / length).astype(BF).astype(F32)
    rest = total - larger
    row = lax.broadcasted_iota(jnp.int32, (2 * LANES, 2 * LANES), 0)
    col = lax.broadcasted_iota(jnp.int32, (2 * LANES, 2 * LANES), 1)
    diagonal = (row == col) & (row % LANES < half)
    for parity in range(2):
        th, tl = ty_ref[parity, 0], ty_ref[parity, 1]
        keep = picked[parity]
        mh = (th.astype(F32) * keep).astype(BF)
        ml = (tl.astype(F32) * keep).astype(BF)
        table = dot_nt(mh, th) + dot_nt(ml, th) + dot_nt(mh, tl)
        value = jnp.where(counts[parity] >= counts[1 - parity], larger, rest)
        if parity:
            value = jnp.where(counts[1] > counts[0], larger, rest)
        h_ref[parity] = jnp.where(diagonal, value, table).astype(BF)


def make_wave(psf_ref, psft_ref, wave_ref, length, classes):
    half = length // 2
    readout = psf_ref.shape[1]
    blank = jnp.zeros((LANES - half, readout), F32)
    psf = jnp.concatenate([psf_ref[:half], blank, psf_ref[half:], blank], 0) * (0.5 / np.pi)
    wide = -(-readout // LANES) * LANES
    if wide > readout:
        psf = jnp.concatenate([psf, jnp.zeros((2 * LANES, wide - readout), F32)], 1)
    for side in range(2):
        psft_ref[side] = psf[side * LANES:(side + 1) * LANES].T
    rows = readout // classes
    for j in range(classes):
        picked = pl.ds(j, rows, stride=classes)
        c, s = turn_pair(jnp.concatenate([psft_ref[0, picked, :], psft_ref[1, picked, :]], 1), WAVE_POLY)
        put(wave_ref.at[j], c.astype(BF), s.astype(BF))


def make_inverse_rows(tx_ref, txt_ref):
    for parity in range(2):
        for part in range(2):
            txt_ref[parity, part] = tx_ref[parity, part].astype(F32).T.astype(BF)


def make_crop(pt_ref, ct_ref, half, classes):
    for j in range(classes):
        back = pt_ref[j].astype(F32).T
        re, im = back[:half], back[half:]
        angle = 2 * np.pi * j / classes
        wr, wi = float(np.cos(angle)), float(np.sin(angle))
        columns = pl.ds(2 * half * j, 2 * half)
        ct_ref[pl.ds(0, half), columns] = re.astype(BF)
        ct_ref[pl.ds(half, half), columns] = (re * wr - im * wi).astype(BF)
        ct_ref[pl.ds(2 * half, half), columns] = im.astype(BF)
        ct_ref[pl.ds(3 * half, half), columns] = (re * wi + im * wr).astype(BF)


def encode(coil, rot_ref, pt_ref, wave_ref, c_ref, w_ref, length, classes):
    width = coil.shape[1]
    half = width // 2
    cr = spread(coil[0], length)
    ci = spread(coil[1], length)
    put(c_ref, cr, ci)
    rr, ri = rot_ref[0, :width], rot_ref[1, :width]
    zr = (cr.astype(F32) * rr - ci.astype(F32) * ri).astype(BF)
    zi = (cr.astype(F32) * ri + ci.astype(F32) * rr).astype(BF)
    ar, ai, br, bi = zr[:half], zi[:half], zr[half:], zi[half:]
    for j in range(classes // 2):
        angle = -2 * np.pi * j / classes
        wr, wi = float(np.cos(angle)), float(np.sin(angle))
        if j == 0:
            ur, ui = br, bi
        else:
            ur, ui = br * wr - bi * wi, br * wi + bi * wr
        for step in range(2):
            cls = j + step * (classes // 2)
            tr, ti = (ar - ur, ai - ui) if step else (ar + ur, ai + ui)
            spectra = dot(pt_ref[cls], jnp.concatenate([tr, ti], 0)).astype(BF)
            sr, si = spectra[:half], spectra[half:]
            c, s = wave_ref[cls, 0, :half], wave_ref[cls, 1, :half]
            vr = sr * c - si * s
            vi = sr * s + si * c
            rows = pl.ds(cls * half, half)
            w_ref[0, rows, :LANES] = vr[:, :LANES] + vr[:, LANES:]
            w_ref[0, rows, LANES:] = vi[:, :LANES] + vi[:, LANES:]
            w_ref[1, rows, :LANES] = vr[:, :LANES] - vr[:, LANES:]
            w_ref[1, rows, LANES:] = vi[:, :LANES] - vi[:, LANES:]


def project(wave_ref, h_ref, w_ref, u_ref, half, classes):
    readout = classes * half
    third = readout // classes
    pieces = [
        (dot(w_ref[0, i:i + third], h_ref[0]).astype(BF), dot(w_ref[1, i:i + third], h_ref[1]).astype(BF))
        for i in range(0, readout, third)
    ]
    for cls in range(classes):
        plus, minus = pieces[cls * half // third]
        rows = slice(cls * half % third, cls * half % third + half)
        for side, y in enumerate((plus[rows] + minus[rows], plus[rows] - minus[rows])):
            lanes = slice(side * LANES, (side + 1) * LANES)
            yr, yi = y[:, :LANES], y[:, LANES:]
            c, s = wave_ref[cls, 0, :half, lanes], wave_ref[cls, 1, :half, lanes]
            u_ref[pl.ds(2 * cls * half, half), lanes] = yr * c + yi * s
            u_ref[pl.ds((2 * cls + 1) * half, half), lanes] = yi * c - yr * s


def decode(acc_ref, ct_ref, c_ref, u_ref, width):
    back = dot(ct_ref[...], u_ref[...])
    br, bi = back[:width].astype(BF), back[width:].astype(BF)
    cr, ci = c_ref[0, :width], c_ref[1, :width]
    acc_ref[0, :width] += (cr * br + ci * bi).astype(F32)
    acc_ref[1, :width] += (cr * bi - ci * br).astype(F32)


def kernel(
    motion_hbm, mask_hbm, image_hbm, tx_hbm, ty_hbm, psf_hbm, pt_hbm, coil_hbm, out_ref,
    motion_ref, mask_ref, image_ref, tx_ref, ty_ref, psf_ref, pt_ref, coil_ref,
    txt_ref, ct_ref, rot_ref, acc_ref, p1_ref, pc_ref, p3_ref, psft_ref, wave_ref, h_ref, c_ref, w_ref, u_ref, sems,
    *, length, classes, unroll,
):
    width = image_ref.shape[1]
    half = length // 2
    sources = (motion_hbm, mask_hbm, image_hbm, tx_hbm, ty_hbm, psf_hbm, pt_hbm)
    targets = (motion_ref, mask_ref, image_ref, tx_ref, ty_ref, psf_ref, pt_ref)
    copies = [pltpu.make_async_copy(a, b, sems.at[i]) for i, (a, b) in enumerate(zip(sources, targets))]
    count = coil_ref.shape[0]
    chunk = 2 - count % 2

    def coil_copy(index):
        part = pl.ds(index * chunk, chunk)
        return pltpu.make_async_copy(coil_hbm.at[part], coil_ref.at[part], sems.at[len(sources) + index])

    for copy in copies:
        copy.start()
    copies[0].wait()
    make_phases(motion_ref, p1_ref, pc_ref, p3_ref, width, length)
    for copy in copies[1:4]:
        copy.wait()
    for index in range(count // chunk):
        coil_copy(index).start()
    make_inverse_rows(tx_ref, txt_ref)
    re, im = spread(image_ref[0], length), spread(image_ref[1], length)
    re, im = shear_rows(re, im, tx_ref, txt_ref, p1_ref, 1.0)
    acc_ref[...] = jnp.zeros_like(acc_ref)
    for copy in copies[4:]:
        copy.wait()
    make_crop(pt_ref, ct_ref, width // 2, classes)
    make_projector(mask_ref, ty_ref, h_ref, length)
    re, im = shear_columns(re, im, ty_ref, pc_ref, 1.0)
    re, im = shear_rows(re, im, tx_ref, txt_ref, p3_ref, 1.0)
    make_wave(psf_ref, psft_ref, wave_ref, length, classes)
    put(rot_ref, re, im)
    for index in range(count // chunk):
        coil_copy(index).wait()

    def run(stage, coil):
        slot = coil % 2 if isinstance(coil, int) else coil[1]
        index = coil if isinstance(coil, int) else coil[0]
        if stage == 0:
            encode(coil_ref[index], rot_ref, pt_ref, wave_ref, c_ref.at[slot], w_ref.at[slot], length, classes)
        elif stage == 1:
            project(wave_ref, h_ref, w_ref.at[slot], u_ref.at[slot], width // 2, classes)
        else:
            decode(acc_ref, ct_ref, c_ref.at[slot], u_ref.at[slot], width)

    def pair(first):
        run(2, (first - 2, 0))
        run(1, (first - 1, 1))
        run(0, (first, 0))
        run(2, (first - 1, 1))
        run(1, (first, 0))
        run(0, (first + 1, 1))

    if count % 2:
        def single(coil, carry):
            for stage in range(3):
                run(stage, (coil, 0))
            return carry

        lax.fori_loop(0, count, single, 0)
    else:
        pairs = count // 2 - 1
        run(0, 0)
        run(1, 0)
        run(0, 1)
        steps = pairs // unroll
        for extra in range(pairs - steps * unroll):
            pair(2 * extra + 2)

        def some_pairs(step, carry):
            for inner in range(unroll):
                pair(2 * (pairs - steps * unroll + step * unroll + inner) + 2)
            return carry

        if steps:
            lax.fori_loop(0, steps, some_pairs, 0)
        run(2, count - 2)
        run(1, count - 1)
        run(2, count - 1)

    re, im = acc_ref[0, :width], acc_ref[1, :width]
    re, im = shear_rows(re, im, tx_ref, txt_ref, p3_ref, -1.0)
    re, im = shear_columns(re, im, ty_ref, pc_ref, -1.0)
    re, im = shear_rows(re, im, tx_ref, txt_ref, p1_ref, -1.0)
    for part, value in enumerate((re, im)):
        out_ref[part] = jnp.concatenate([value[:, :half], value[:, LANES:LANES + half]], 1)


def slice_operator(motion, mask, image, psf, coils):
    _, width, length = image.shape
    readout = psf.shape[1]
    classes = readout // (width // 2)
    pads = readout_tables(width, readout)
    tx, ty = row_tables(width), column_tables(length)
    wide = -(-readout // LANES) * LANES
    operands = (motion, mask, image, jnp.asarray(tx), jnp.asarray(ty), psf, jnp.asarray(pads), coils)
    return pl.pallas_call(
        functools.partial(kernel, length=length, classes=classes, unroll=UNROLL),
        in_specs=[pl.BlockSpec(memory_space=pltpu.HBM) for _ in operands],
        out_specs=pl.BlockSpec(memory_space=pltpu.VMEM),
        out_shape=jax.ShapeDtypeStruct(image.shape, F32),
        scratch_shapes=[pltpu.SMEM(motion.shape, motion.dtype)]
        + [pltpu.VMEM(a.shape, a.dtype) for a in operands[1:]]
        + [
            pltpu.VMEM(tx.shape, BF),
            pltpu.VMEM((2 * width, classes * width), BF),
            pltpu.VMEM((2, width + 8, 2 * LANES), F32),
            pltpu.VMEM((2, width + 8, 2 * LANES), F32),
            pltpu.VMEM((2, width + 8, 2 * LANES), F32),
            pltpu.VMEM((2, 2, width + 8, LANES), F32),
            pltpu.VMEM((2, width + 8, 2 * LANES), F32),
            pltpu.VMEM((2, wide, LANES), F32),
            pltpu.VMEM((classes, 2, width // 2 + 16, 2 * LANES), BF),
            pltpu.VMEM((2, 2 * LANES, 2 * LANES), BF),
            pltpu.VMEM((2, 2, width + 16, 2 * LANES), BF),
            pltpu.VMEM((2, 2, readout + 16, 2 * LANES), BF),
            pltpu.VMEM((2, 2 * readout, 2 * LANES), BF),
            pltpu.SemaphoreType.DMA((len(operands) + coils.shape[0],)),
        ],
        compiler_params=pltpu.CompilerParams(vmem_limit_bytes=40 * 2**20),
        name="normal_operator",
    )(*[pltpu.with_memory_space_constraint(a, pltpu.HBM) for a in operands])


def from_partner(value, axis, apart):
    mask = 2**apart
    pairs = [(source, source ^ mask) for source in range(lax.axis_size(axis))]
    return lax.ppermute(value, axis, pairs)


def gather_slice(values, bit_count, device_rank):
    for bit_index in range(bit_count):
        partner = from_partner(values, "space", bit_index)
        low_side = device_rank >> bit_index & 1 == 0
        values = jnp.where(
            low_side, jnp.concatenate([values, partner], 0), jnp.concatenate([partner, values], 0)
        )
    return values


def sum_slice(values, bit_count, device_rank):
    for bit_index in reversed(range(bit_count)):
        half_rows = values.shape[0] // 2
        low_side = device_rank >> bit_index & 1 == 0
        kept_part = jnp.where(low_side, values[:half_rows], values[half_rows:])
        sent_part = jnp.where(low_side, values[half_rows:], values[:half_rows])
        values = kept_part + from_partner(sent_part, "space", bit_index)
    return values


def regroup_coils(coil_maps, bit_count, device_rank):
    group_size = 1 << bit_count
    pieces = coil_maps.reshape((group_size, coil_maps.shape[0] // group_size) + coil_maps.shape[1:])
    for bit_index in range(bit_count):
        old_shape = pieces.shape
        halves = pieces.reshape((group_size >> bit_index + 1, 2, 1 << bit_index) + old_shape[1:])
        low_side = device_rank >> bit_index & 1 == 0
        kept_part = jnp.where(low_side, halves[:, 0], halves[:, 1])
        sent_part = jnp.where(low_side, halves[:, 1], halves[:, 0])
        partner = from_partner(sent_part, "space", bit_index)
        pieces = jnp.stack(
            [jnp.where(low_side, kept_part, partner), jnp.where(low_side, partner, kept_part)], 1
        ).reshape(old_shape)
    moved = jnp.moveaxis(pieces, 0, 1)
    return moved.reshape((moved.shape[0], group_size * coil_maps.shape[1]) + coil_maps.shape[2:])


def on_device(image, coil_maps, psf_phase, line_mask, motion):
    lines = image.shape[0]
    length = line_mask.shape[1]
    device_rank = lax.axis_index("space")
    group_size = max(1, length // lines)
    bit_count = group_size.bit_length() - 1
    if bit_count:
        coil_maps = regroup_coils(coil_maps, bit_count, device_rank)
        psf_phase = gather_slice(psf_phase, bit_count, device_rank)
        image = gather_slice(image, bit_count, device_rank)
    image = jnp.transpose(image, (1, 2, 0))
    coil_maps = jnp.transpose(coil_maps, (0, 2, 3, 1))
    results = []
    for start in range(0, image.shape[2], length):
        stop = start + length
        results.append(
            slice_operator(
                motion, line_mask, image[:, :, start:stop], psf_phase[start:stop], coil_maps[..., start:stop]
            )
        )
    result = results[0] if len(results) == 1 else jnp.concatenate(results, 2)
    if bit_count:
        result = jnp.transpose(result, (2, 0, 1))
        result = sum_slice(result, bit_count, device_rank)
        result = jnp.transpose(result, (1, 2, 0))
    shots = lax.axis_size("shot")
    total = result
    for apart in range(1, shots):
        pairs = [(source, (source + apart) % shots) for source in range(shots)]
        total = total + lax.ppermute(result, "shot", pairs)
    return jnp.transpose(total, (2, 0, 1))


def solution(mesh):
    in_specs = (
        P(("parts", "space"), None, None),
        P(None, ("parts", "space"), None, None),
        P(("parts", "space"), None),
        P(("parts", "shot"), None),
        P(("parts", "shot"), None),
    )
    out_specs = P(("parts", "space"), None, None)
    return jax.shard_map(
        on_device, mesh=mesh, in_specs=in_specs, out_specs=out_specs, check_vma=False
    )
```
